32 devices in a mesh: groups: 2 (over x), ctx: 16 (over z, y, core), tp: 1.
Axes of the slice: x: 2, y: 2, z: 4, core: 2. Of those that a mesh axis runs over, the one named last changes fastest.
Arguments:
- query_states: bfloat16 [8192, 32, 128], P(('groups', 'ctx'), 'tp'), parts along dimension 0, may hold values from -8 to 8
- key_states: bfloat16 [8192, 4, 128], P(('groups', 'ctx'), 'tp'), parts along dimension 0, may hold values from -8 to 8
- value_rows: bfloat16 [8192, 4, 128], P(('groups', 'ctx'), 'tp'), parts along dimension 0, may hold values from -12 to 12
- positions: int32 [8192], P(('groups', 'ctx')), parts along dimension 0, may hold values from 0 to 4095, as said below
- out_weight: bfloat16 [4096, 4096], P('tp', 'ctx'), may hold values from -0.375 to 0.375
Outputs:
- projected: bfloat16 [8192, 4096], P(('groups', 'ctx'), 'tp'), parts along dimension 0
The draws below stay inside these ranges and needn't reach their ends.
There are 2 independent parts, one for each index of `groups`. The reference program is written for one: setup_inputs(seed, part) draws one part's arguments, and reference() takes and returns one part's arrays. A program takes and returns all parts, laid end to end along the dimension named above; an argument that names none is the same for every part. Nothing has to cross between parts.
Inputs may be any that keep to these rules, and one draw needn't show every extreme that they name: Each of 0 to 4095 appears once. Half-block b holds positions b * 128 to (b + 1) * 128 - 1. The 256 rows of one device along ctx hold half-block j and then half-block 32 - 1 - j, each in rising order, for a j below 16 that differs from device to device.
All inputs are finite; a program needn't handle non-finite values.
Results may differ from the reference program's by a relative error of at most 0.01.
Values may be sent and summed in bfloat16 or wider, within the bound.
A program may use at most 128 MiB of HBM per device.

```python
from functools import partial
import jax
import jax.numpy as jnp
from jax import lax

QUERY_HEAD_COUNT = 32
KEY_VALUE_HEADS = 4
HEAD_WIDTH = 128
DOUT = 4096
HALF = 128
SEQUENCE_LENGTH = 4096
HALF_BLOCK_COUNT = 32


def draw_query_states(key, part):
    base_point = jax.random.fold_in(key, 21)
    value_entries = jnp.clip(jax.random.normal(jax.random.fold_in(base_point, 1), (SEQUENCE_LENGTH, QUERY_HEAD_COUNT, HEAD_WIDTH)), -8.0, 8.0)
    return value_entries.astype(jnp.bfloat16)


def draw_key_states(key, part):
    base_point = jax.random.fold_in(key, 41)
    value_entries = jnp.clip(jax.random.normal(jax.random.fold_in(base_point, 1), (SEQUENCE_LENGTH, KEY_VALUE_HEADS, HEAD_WIDTH)), -8.0, 8.0)
    return value_entries.astype(jnp.bfloat16)


def draw_positions(key, part):
    order = jax.random.permutation(jax.random.fold_in(key, 31), HALF_BLOCK_COUNT // 2)
    within = jnp.arange(HALF)
    lower = order[:, None] * HALF + within[None, :]
    upper = (HALF_BLOCK_COUNT - 1 - order)[:, None] * HALF + within[None, :]
    return jnp.concatenate([lower, upper], axis=1).reshape(SEQUENCE_LENGTH).astype(jnp.int32)


def steps_of(stream_key, dims, cuts, low, top_value):
    loudness = 1.0
    for dim, parts in cuts:
        steps = jax.random.uniform(jax.random.fold_in(jax.random.fold_in(stream_key, 6), dim), (parts,), jnp.float32, low / len(cuts), top_value / len(cuts))
        loudness = loudness * jnp.repeat(jnp.exp(steps), dims[dim] // parts).reshape((-1,) + (1,) * (len(dims) - 1 - dim))
    return loudness


def gaussian(key, shape, scale, limit, shards=(), dtype=jnp.bfloat16):
    loudness = steps_of(key, shape, shards, -0.22, 0.18) if shards else 1.0
    values = jax.random.normal(key, shape, jnp.float32) * scale * loudness
    return jnp.minimum(jnp.maximum(values, -limit), limit).astype(dtype)


def setup_inputs(seed: int = 0, part: int = 0) -> dict:
    streams_of = jax.random.split(jax.random.key(seed), 6)
    part_splits = jax.random.split(jax.random.fold_in(streams_of[5], part), 6)
    query_states = draw_query_states(jax.random.fold_in(jax.random.fold_in(streams_of[5], part), 71), part)
    key_states = draw_key_states(jax.random.fold_in(jax.random.fold_in(streams_of[5], part), 71), part)
    value_rows = gaussian(part_splits[2], (SEQUENCE_LENGTH, KEY_VALUE_HEADS, HEAD_WIDTH), 2.0, 12.0, ((0, 16),))
    positions = draw_positions(jax.random.fold_in(jax.random.fold_in(streams_of[5], part), 71), part)
    out_weight = gaussian(streams_of[4], (QUERY_HEAD_COUNT * HEAD_WIDTH, DOUT), (QUERY_HEAD_COUNT * HEAD_WIDTH // 16) ** -0.5, 0.375, ((1, 16),))
    return {"query_states": query_states, "key_states": key_states, "value_rows": value_rows, "positions": positions, "out_weight": out_weight}


def one_head(operands, visible):
    query_head, key_head, value_head = operands
    scores = jnp.dot(query_head, key_head.T, preferred_element_type=jnp.float32) * (HEAD_WIDTH ** -0.5)
    scores = jnp.where(visible, scores, -jnp.inf)
    largest = jnp.max(scores, axis=1)
    exp_scores = jnp.exp(scores - largest[:, None])
    denominator = jnp.sum(exp_scores, axis=1)
    weighted = jnp.dot(exp_scores.astype(jnp.bfloat16), value_head, preferred_element_type=jnp.float32)
    return (weighted / denominator[:, None]).astype(jnp.bfloat16)


def reference(query_states, key_states, value_rows, positions, out_weight):
    visible = positions[None, :] <= positions[:, None]
    group_width = QUERY_HEAD_COUNT // KEY_VALUE_HEADS
    query_major = jnp.moveaxis(query_states, 1, 0)
    key_major = jnp.repeat(jnp.moveaxis(key_states, 1, 0), group_width, axis=0)
    value_major = jnp.repeat(jnp.moveaxis(value_rows, 1, 0), group_width, axis=0)
    attended = lax.map(partial(one_head, visible=visible), (query_major, key_major, value_major))
    attended = jnp.moveaxis(attended, 0, 1).reshape(SEQUENCE_LENGTH, QUERY_HEAD_COUNT * HEAD_WIDTH)
    return jnp.dot(attended, out_weight, preferred_element_type=jnp.float32).astype(jnp.bfloat16)
```

```python
import functools
import math

import jax
import jax.numpy as jnp
from jax import lax
from jax.experimental import pallas as pl
from jax.experimental.pallas import tpu as pltpu
from jax.sharding import PartitionSpec as P

LOW_START = -1e30
BLOCKS_PER_STEP = 4
CHUNK = 1024
TAIL = 16


def attend_kernel(half, group, place_ref, own_ref, q_ref, k_ref, v_ref, out_ref, acc_ref, max_ref, sum_ref):
    rows = group * half
    head_size = q_ref.shape[-1]
    span = BLOCKS_PER_STEP * half
    chunk = min(CHUNK, rows)
    to_exp2 = head_size ** (-0.5) * math.log2(math.e)

    def step(which, number, masked, query_block):
        keys, values = [], []
        for i in range(BLOCKS_PER_STEP):
            place = place_ref[number * BLOCKS_PER_STEP + i]
            keys.append(k_ref[pl.ds(pl.multiple_of(place, TAIL), half), :])
            values.append(v_ref[pl.ds(pl.multiple_of(place, TAIL), half), :])
        key_part = jnp.concatenate(keys, axis=0)
        value_part = jnp.concatenate(values, axis=0)
        if masked:
            key_place = number * span + lax.broadcasted_iota(jnp.int32, (span, chunk), 0)
            query_place = query_block * half + lax.broadcasted_iota(jnp.int32, (span, chunk), 1) % half
            visible = key_place <= query_place
        for c in range(rows // chunk):
            cols = pl.ds(c * chunk, chunk)
            scores = lax.dot_general(
                key_part,
                q_ref[0, which, cols, :],
                (((1,), (1,)), ((), ())),
                preferred_element_type=jnp.float32,
            )
            if masked:
                scores = jnp.where(visible, scores, LOW_START)
            old_max = max_ref[:, cols]
            new_max = jnp.maximum(old_max, jnp.max(scores, axis=0, keepdims=True))
            factor = jnp.exp2((old_max - new_max) * to_exp2)
            exp_scores = jnp.exp2((scores - new_max) * to_exp2)
            max_ref[:, cols] = new_max
            sum_ref[:, cols] = sum_ref[:, cols] * factor + jnp.sum(exp_scores, axis=0, keepdims=True)
            weighted = lax.dot_general(
                value_part,
                exp_scores.astype(jnp.bfloat16),
                (((0,), (0,)), ((), ())),
                preferred_element_type=jnp.float32,
            )
            acc_ref[:, cols] = acc_ref[:, cols] * factor + weighted

    for which in range(2):
        query_block = own_ref[which]
        steps = query_block // BLOCKS_PER_STEP
        max_ref[...] = jnp.full_like(max_ref, LOW_START)
        sum_ref[...] = jnp.zeros_like(sum_ref)
        acc_ref[...] = jnp.zeros_like(acc_ref)

        @pl.loop(0, steps)
        def _(number):
            step(which, number, False, query_block)

        step(which, steps, True, query_block)
        for g in range(group):
            cols = pl.ds(g * half, half)
            attended = acc_ref[:, cols] / sum_ref[:, cols]
            out_ref[pl.ds(g * head_size, head_size), pl.ds(which * half, half)] = attended.astype(jnp.bfloat16)


def attend(query_parts, gathered, place, own, first_head, all_heads, half):
    kv_heads, _, rows, head_size = query_parts.shape
    keys_total = gathered.shape[0]
    blocks = place.shape[0]
    group = rows // half
    flops = 4 * kv_heads * rows * head_size * half * (blocks + 1)
    return pl.pallas_call(
        functools.partial(attend_kernel, half, group),
        out_shape=jax.ShapeDtypeStruct((kv_heads * group * head_size, 2 * half), jnp.bfloat16),
        grid_spec=pltpu.PrefetchScalarGridSpec(
            num_scalar_prefetch=2,
            grid=(kv_heads,),
            in_specs=[
                pl.BlockSpec((1, 2, rows, head_size), lambda h, *_: (h, 0, 0, 0)),
                pl.BlockSpec((keys_total, head_size), lambda h, *_: (0, h + first_head)),
                pl.BlockSpec((keys_total, head_size), lambda h, *_: (0, h + first_head + all_heads)),
            ],
            out_specs=pl.BlockSpec((group * head_size, 2 * half), lambda h, *_: (h, 0)),
            scratch_shapes=[
                pltpu.VMEM((head_size, rows), jnp.float32),
                pltpu.VMEM((1, rows), jnp.float32),
                pltpu.VMEM((1, rows), jnp.float32),
            ],
        ),
        compiler_params=pltpu.CompilerParams(
            dimension_semantics=("arbitrary",), vmem_limit_bytes=20 * 1024 * 1024
        ),
        cost_estimate=pl.CostEstimate(
            flops=flops, bytes_accessed=2 * gathered.size, transcendentals=flops // (4 * head_size)
        ),
        name="attend",
    )(place, own, query_parts, gathered, gathered)


def spread_kernel(devices, own_ref, out_ref, far_send, far_recv, side_send, side_recv, pair_send, pair_recv, own_sem):
    me = lax.axis_index("ctx")
    outers = devices // 4
    outer, middle, inner = me // 4, (me // 2) % 2, me % 2

    def at(o, m, i):
        return (o * 2 + m) * 2 + i

    side = at(outer, 1 - middle, inner)
    pair = at(outer, middle, 1 - inner)
    far = [at((outer + k) % outers, middle, inner) for k in range(1, outers)]
    barrier = pltpu.get_barrier_semaphore()
    for other in far + [side, pair]:
        pl.semaphore_signal(barrier, inc=1, device_id={"ctx": other}, device_id_type=pl.DeviceIdType.MESH)
    pl.semaphore_wait(barrier, outers + 1)

    def send(source, slot, sends, recvs, number, target):
        return pltpu.make_async_remote_copy(
            src_ref=source,
            dst_ref=out_ref.at[slot],
            send_sem=sends.at[number],
            recv_sem=recvs.at[number],
            device_id={"ctx": target},
            device_id_type=pl.DeviceIdType.MESH,
        )

    own = pltpu.make_async_copy(own_ref, out_ref.at[me], own_sem)
    far_copies = [send(own_ref, me, far_send, far_recv, k, far[k]) for k in range(outers - 1)]
    for copy in far_copies:
        copy.start()
    side_copies = [send(own_ref, me, side_send, side_recv, 0, side)]
    pair_copies = [send(own_ref, me, pair_send, pair_recv, 0, pair)]
    side_copies[0].start()
    pair_copies[0].start()
    own.start()
    for k in range(outers - 1):
        far_copies[k].wait_recv()
        slot = at((outer + outers - 1 - k) % outers, middle, inner)
        side_copies.append(send(out_ref.at[slot], slot, side_send, side_recv, k + 1, side))
        pair_copies.append(send(out_ref.at[slot], slot, pair_send, pair_recv, k + 1, pair))
        side_copies[-1].start()
        pair_copies[-1].start()
    for k in range(outers):
        side_copies[k].wait_recv()
        slot = at((outer + outers - k) % outers, 1 - middle, inner)
        pair_copies.append(send(out_ref.at[slot], slot, pair_send, pair_recv, outers + k, pair))
        pair_copies[-1].start()
    for copy in pair_copies:
        copy.wait_recv()
    for copy in far_copies + side_copies + pair_copies:
        copy.wait_send()
    own.wait()


def spread(packed):
    devices = lax.axis_size("ctx")
    outers = devices // 4
    rows, columns = packed.shape
    gathered = pl.pallas_call(
        functools.partial(spread_kernel, devices),
        out_shape=jax.ShapeDtypeStruct((devices, rows, columns), packed.dtype),
        in_specs=[pl.BlockSpec(memory_space=pltpu.VMEM)],
        out_specs=pl.BlockSpec(memory_space=pltpu.VMEM),
        scratch_shapes=[
            pltpu.SemaphoreType.DMA((outers - 1,)),
            pltpu.SemaphoreType.DMA((outers - 1,)),
            pltpu.SemaphoreType.DMA((outers,)),
            pltpu.SemaphoreType.DMA((outers,)),
            pltpu.SemaphoreType.DMA((2 * outers,)),
            pltpu.SemaphoreType.DMA((2 * outers,)),
            pltpu.SemaphoreType.DMA,
        ],
        compiler_params=pltpu.CompilerParams(
            collective_id=0, has_side_effects=True, vmem_limit_bytes=24 * 1024 * 1024
        ),
        cost_estimate=pl.CostEstimate(flops=0, bytes_accessed=20 * packed.size * devices, transcendentals=0),
        name="spread",
    )(packed)
    return gathered


def hand_on(value, by):
    parts = lax.axis_size("groups")
    return lax.ppermute(value, "groups", [(i, (i + by) % parts) for i in range(parts)])


def weave_kernel(share, me_ref, *refs):
    *shares, out_ref = refs
    parts = len(shares)
    for p in range(parts):
        by = lax.rem(p - me_ref[0] + parts, parts)
        chosen = shares[0][...]
        for k in range(1, parts):
            chosen = jnp.where(by == k, shares[k][...], chosen)
        for i in range(chosen.shape[1] // share):
            out_ref[:, (i * parts + p) * share : (i * parts + p + 1) * share] = chosen[:, i * share : (i + 1) * share]


def weave(results, me_part, devices):
    parts = len(results)
    tokens, columns = results[0].shape
    share = columns // devices
    return pl.pallas_call(
        functools.partial(weave_kernel, share),
        out_shape=jax.ShapeDtypeStruct((tokens, parts * columns), results[0].dtype),
        grid_spec=pltpu.PrefetchScalarGridSpec(
            num_scalar_prefetch=1,
            grid=(devices // 4,),
            in_specs=[pl.BlockSpec((tokens, 4 * share), lambda i, *_: (0, i))] * parts,
            out_specs=pl.BlockSpec((tokens, 4 * parts * share), lambda i, *_: (0, i)),
        ),
        name="weave",
    )(me_part.astype(jnp.int32).reshape(1), *results)


def layer_kernel(sizes, first_ref, table_ref, kv_ref, q_ref, w_ref, out_ref, *scratch):
    devices, half, kv_heads, group, head_size, share = sizes
    (kv_all, firsts, place_vec, place_ref, w_all, acc_ref, max_ref, sum_ref, rows_ref, back_ref, *sems) = scratch
    (far_send, far_recv, side_send, side_recv, pair_send, pair_recv) = sems[:6]
    (wfar_send, wfar_recv, wside_send, wside_recv, wpair_send, wpair_recv) = sems[6:12]
    (rows_send, rows_recv, back_send, back_recv, own_sem, place_sem) = sems[12:]
    outers = devices // 4
    blocks = 2 * devices
    tokens = 2 * half
    width = group * half
    depth = kv_heads * group * head_size
    pieces = kv_heads
    piece = depth // pieces
    span = BLOCKS_PER_STEP * half
    low_groups = devices // BLOCKS_PER_STEP
    steps = low_groups + 1
    to_exp2 = head_size ** (-0.5) * math.log2(math.e)

    part = lax.axis_index("groups")
    me = lax.axis_index("ctx")
    outer, middle, inner = me // 4, (me // 2) % 2, me % 2

    def flip(number, by):
        result, unit = 0, 1
        while unit < outers:
            result = result + (number // unit + by // unit) % 2 * unit
            unit *= 2
        return result

    def slot_of(hop, cross, swap):
        return (flip(outer, hop) * 2 + (middle + cross) % 2) * 2 + (inner + swap) % 2

    far = [slot_of(k, 0, 0) for k in range(outers)]
    side = slot_of(0, 1, 0)
    pair = slot_of(0, 0, 1)
    guest = lax.rem(part + 1, 2)

    barrier = pltpu.get_barrier_semaphore()
    for other in far[1:] + [side, pair]:
        pl.semaphore_signal(barrier, inc=1, device_id={"ctx": other}, device_id_type=pl.DeviceIdType.MESH)
    pl.semaphore_signal(barrier, inc=1, device_id={"groups": guest}, device_id_type=pl.DeviceIdType.MESH)
    pl.semaphore_wait(barrier, outers + 2)

    def remote(source, target, send, recv, axis, index):
        return pltpu.make_async_remote_copy(
            src_ref=source,
            dst_ref=target,
            send_sem=send,
            recv_sem=recv,
            device_id={axis: index},
            device_id_type=pl.DeviceIdType.MESH,
        )

    def own_item(item):
        return table_ref if item == 0 else kv_ref.at[pl.ds((item - 1) * half, half), :]

    def item_at(item, slot):
        if item == 0:
            return firsts.at[slot]
        return kv_all.at[slot * 2 + item - 1]

    def source_of(item, hop, cross):
        return own_item(item) if hop == 0 and cross == 0 else item_at(item, slot_of(hop, cross, 0))

    def far_copy(item, hop):
        return remote(own_item(item), item_at(item, me), far_send.at[item, hop], far_recv.at[item, hop], "ctx", far[hop])

    def side_copy(item, hop):
        return remote(
            source_of(item, hop, 0), item_at(item, far[hop]), side_send.at[item, hop], side_recv.at[item, hop], "ctx", side
        )

    def pair_copy(item, hop, cross):
        n = hop * 2 + cross
        return remote(
            source_of(item, hop, cross),
            item_at(item, slot_of(hop, cross, 0)),
            pair_send.at[item, n],
            pair_recv.at[item, n],
            "ctx",
            pair,
        )

    def w_at(slot, n):
        return w_all.at[slot, pl.ds(n * piece, piece), :]

    def wfar_copy(hop, n):
        return remote(w_at(me, n), w_at(me, n), wfar_send.at[hop, n], wfar_recv.at[hop, n], "ctx", far[hop])

    def wside_copy(hop, n):
        ref = w_at(far[hop], n)
        return remote(ref, ref, wside_send.at[hop, n], wside_recv.at[hop, n], "ctx", side)

    def wpair_copy(hop, cross, n):
        ref = w_at(slot_of(hop, cross, 0), n)
        return remote(ref, ref, wpair_send.at[hop * 2 + cross, n], wpair_recv.at[hop * 2 + cross, n], "ctx", pair)

    def rows_copy(h):
        cols = pl.ds(pl.multiple_of(h * piece, piece), piece)
        return remote(
            rows_ref.at[pl.ds(0, tokens), cols],
            rows_ref.at[pl.ds(tokens, tokens), cols],
            rows_send.at[h],
            rows_recv.at[h],
            "groups",
            guest,
        )

    def back_copy(n, slot):
        cols = pl.ds(pl.multiple_of((slot * 2 + part) * share, share), share)
        return remote(back_ref.at[n], out_ref.at[:, cols], back_send.at[n], back_recv.at[n], "groups", guest)

    def far_arrived(item, hop):
        far_copy(item, hop).wait_recv()
        side_copy(item, hop).start()
        pair_copy(item, hop, 0).start()

    def side_arrived(item, hop):
        side_copy(item, hop).wait_recv()
        pair_copy(item, hop, 1).start()

    def pair_arrived(item, hop):
        for cross in range(2):
            pair_copy(item, hop, cross).wait_recv()

    def wfar_arrived(hop, n):
        wfar_copy(hop, n).wait_recv()
        wside_copy(hop, n).start()
        wpair_copy(hop, 0, n).start()

    def wside_arrived(hop, n):
        wside_copy(hop, n).wait_recv()
        wpair_copy(hop, 1, n).start()

    own_weight = pltpu.make_async_copy(
        w_ref.at[:, pl.ds(pl.multiple_of(part * share, share), share)], w_all.at[me], own_sem
    )
    own_weight.start()
    for item in range(3):
        for hop in range(1, outers):
            far_copy(item, hop).start()
        if item < 2:
            side_copy(item, 0).start()
        pair_copy(item, 0, 0).start()
    for i in range(2):
        kv_all[me * 2 + i] = kv_ref[i * half : (i + 1) * half, :]
    firsts[me] = table_ref[...]
    for h in range(kv_heads):
        max_ref[h * (steps + 1)] = jnp.full(max_ref.shape[1:], LOW_START, jnp.float32)
        sum_ref[h * (steps + 1)] = jnp.zeros(sum_ref.shape[1:], jnp.float32)
        acc_ref[h * (steps + 1)] = jnp.zeros(acc_ref.shape[1:], jnp.float32)
    own_weight.wait()
    for hop in range(1, outers):
        for n in range(pieces):
            wfar_copy(hop, n).start()

    def step(h, which, places, old, new, reset, visible):
        keys = pl.ds(pl.multiple_of(h * head_size, head_size), head_size)
        values = pl.ds(pl.multiple_of((kv_heads + h) * head_size, head_size), head_size)
        key_part = jnp.concatenate([kv_all[p, :, keys] for p in places], axis=0)
        value_part = jnp.concatenate([kv_all[p, :, values] for p in places], axis=0)
        scores = lax.dot_general(
            key_part, q_ref[h, which], (((1,), (1,)), ((), ())), preferred_element_type=jnp.float32
        )
        old_max = max_ref[old]
        if visible is not None:
            scores = jnp.where(visible, scores, LOW_START)
            old_max = jnp.where(reset, LOW_START, old_max)
        new_max = jnp.maximum(old_max, jnp.max(scores, axis=0, keepdims=True))
        factor = jnp.exp2((old_max - new_max) * to_exp2)
        exp_scores = jnp.exp2((scores - new_max) * to_exp2)
        max_ref[new] = new_max
        sum_ref[new] = sum_ref[old] * factor + jnp.sum(exp_scores, axis=0, keepdims=True)
        weighted = lax.dot_general(
            value_part,
            exp_scores.astype(jnp.bfloat16),
            (((0,), (0,)), ((), ())),
            preferred_element_type=jnp.float32,
        )
        acc_ref[new] = acc_ref[old] * factor + weighted

    def low_blocks(hop):
        start = flip(outer, hop) * 4

        @pl.loop(0, kv_heads)
        def _(h):
            at = h * (steps + 1)
            step(h, 1, [(start + i) * 2 for i in range(4)], at, at, None, None)

    for item in range(2):
        side_arrived(item, 0)
        far_arrived(item, 1)
    side_copy(2, 0).start()
    for item in range(2):
        pair_arrived(item, 0)
    low_blocks(0)
    for item in range(2):
        for hop in range(2, outers):
            far_arrived(item, hop)
            side_arrived(item, hop - 1)
        side_arrived(item, outers - 1)
    far_arrived(2, 1)
    side_arrived(2, 0)
    for hop in range(1, outers):
        for item in range(2):
            pair_arrived(item, hop)
        if hop == outers - 1:
            lanes = lax.broadcasted_iota(jnp.int32, firsts.shape[1:], 1)
            places = jnp.zeros(firsts.shape[1:], jnp.int32)
            for d in range(devices):
                places = places + jnp.where(firsts[d] == lanes, d * 2, 0)
                places = places + jnp.where(blocks - 1 - firsts[d] == lanes, d * 2 + 1, 0)
            place_vec[...] = jnp.minimum(places, blocks - 1)
        low_blocks(hop)
        if hop + 1 < outers:
            far_arrived(2, hop + 1)
        side_arrived(2, hop)
    to_scalars = pltpu.make_async_copy(place_vec, place_ref, place_sem)
    to_scalars.start()
    for n in range(pieces):
        wside_copy(0, n).start()
        wpair_copy(0, 0, n).start()
    for hop in range(outers):
        pair_arrived(2, hop)
    to_scalars.wait()

    first = first_ref[0]
    upper_steps = (devices - 1 - first) // BLOCKS_PER_STEP + 1
    key_rows = lax.broadcasted_iota(jnp.int32, (span, width), 0)
    query_cols = lax.broadcasted_iota(jnp.int32, (span, width), 1) % half

    @pl.loop(0, kv_heads)
    def _(h):
        wfar_copy(1, h).wait_recv()
        wside_copy(1, h).start()
        wpair_copy(1, 0, h).start()

        @pl.loop(0, steps)
        def _(t):
            upper = t < upper_steps
            number = jnp.where(upper, low_groups + t, t - upper_steps)
            block = jnp.where(upper, blocks - 1 - first, first)
            which = jnp.where(upper, 1, 0)
            places = [place_ref[0, number * BLOCKS_PER_STEP + i] for i in range(BLOCKS_PER_STEP)]
            visible = number * span + key_rows <= block * half + query_cols
            at = h * (steps + 1) + t
            step(h, which, places, at, at + 1, t == upper_steps, visible)

        for which in range(2):
            at = h * (steps + 1) + (upper_steps if which == 1 else steps)
            for g in range(group):
                cols = pl.ds(g * half, half)
                attended = acc_ref[at, :, cols] / sum_ref[at, :, cols]
                target = pl.ds(pl.multiple_of(h * piece + g * head_size, head_size), head_size)
                rows_ref[pl.ds(which * half, half), target] = attended.T.astype(jnp.bfloat16)
        rows_copy(h).start()

    for n in range(pieces):
        wside_arrived(0, n)
    for n in range(pieces):
        wfar_arrived(2, n)
    for n in range(pieces):
        wside_arrived(1, n)
    for h in range(kv_heads):
        rows_copy(h).wait_recv()

    def project(hop, cross):
        n = hop * 2 + cross
        base = slot_of(hop, cross, 0) - inner
        for m in range(pieces):
            wpair_copy(hop, cross, m).wait_recv()
        weight = jnp.concatenate([w_all[base], w_all[base + 1]], axis=1)
        product = lax.dot_general(
            rows_ref[...], weight, (((1,), (0,)), ((), ())), preferred_element_type=jnp.float32
        ).astype(jnp.bfloat16)
        for i in range(2):
            back_ref[n * 2 + i] = product[tokens:, i * share : (i + 1) * share]
        for i in range(2):
            cols = pl.ds(pl.multiple_of(((base + i) * 2 + part) * share, share), share)
            out_ref[:, cols] = product[:tokens, i * share : (i + 1) * share]
        for i in range(2):
            back_copy(n * 2 + i, base + i).start()

    project(0, 0)
    project(0, 1)
    for n in range(pieces):
        wfar_arrived(3, n)
    for n in range(pieces):
        wside_arrived(2, n)
    project(1, 0)
    project(1, 1)
    project(2, 0)
    project(2, 1)
    for n in range(pieces):
        wside_arrived(3, n)
    project(3, 0)
    project(3, 1)

    for n in range(2 * 2 * outers):
        back_copy(n, 0).wait_recv()
    for n in range(2 * 2 * outers):
        back_copy(n, 0).wait_send()
    for h in range(kv_heads):
        rows_copy(h).wait_send()
    for hop in range(outers):
        for item in range(3):
            if hop:
                far_copy(item, hop).wait_send()
            side_copy(item, hop).wait_send()
            for cross in range(2):
                pair_copy(item, hop, cross).wait_send()
        for n in range(pieces):
            if hop:
                wfar_copy(hop, n).wait_send()
            wside_copy(hop, n).wait_send()
            for cross in range(2):
                wpair_copy(hop, cross, n).wait_send()


def layer(query_parts, packed, first, out_weight, half):
    devices = lax.axis_size("ctx")
    outers = devices // 4
    kv_heads, _, width, head_size = query_parts.shape
    group = width // half
    tokens = 2 * half
    depth, columns = out_weight.shape
    share = columns // 2
    steps = devices // BLOCKS_PER_STEP + 1
    slots = kv_heads * (steps + 1)
    pieces = kv_heads
    table = jnp.full((8, 128), first, jnp.int32)
    dma = pltpu.SemaphoreType.DMA
    flops = 4 * query_parts.size * half * (2 * devices + 1) // 2 + 4 * tokens * depth * columns * devices // 2
    return pl.pallas_call(
        functools.partial(layer_kernel, (devices, half, kv_heads, group, head_size, share)),
        out_shape=jax.ShapeDtypeStruct((tokens, columns * devices), jnp.bfloat16),
        in_specs=[
            pl.BlockSpec(memory_space=pltpu.SMEM),
            pl.BlockSpec(memory_space=pltpu.VMEM),
            pl.BlockSpec(memory_space=pltpu.VMEM),
            pl.BlockSpec(memory_space=pltpu.VMEM),
            pl.BlockSpec(memory_space=pl.ANY),
        ],
        out_specs=pl.BlockSpec(memory_space=pltpu.VMEM),
        scratch_shapes=[
            pltpu.VMEM((2 * devices, half, packed.shape[1]), packed.dtype),
            pltpu.VMEM((devices, 8, 128), jnp.int32),
            pltpu.VMEM((8, 128), jnp.int32),
            pltpu.SMEM((8, 128), jnp.int32),
            pltpu.VMEM((devices, depth, share), out_weight.dtype),
            pltpu.VMEM((slots, head_size, width), jnp.float32),
            pltpu.VMEM((slots, 1, width), jnp.float32),
            pltpu.VMEM((slots, 1, width), jnp.float32),
            pltpu.VMEM((2 * tokens, depth), jnp.bfloat16),
            pltpu.VMEM((devices, tokens, share), jnp.bfloat16),
            dma((3, outers)),
            dma((3, outers)),
            dma((3, outers)),
            dma((3, outers)),
            dma((3, 2 * outers)),
            dma((3, 2 * outers)),
            dma((outers, pieces)),
            dma((outers, pieces)),
            dma((outers, pieces)),
            dma((outers, pieces)),
            dma((2 * outers, pieces)),
            dma((2 * outers, pieces)),
            dma((kv_heads,)),
            dma((kv_heads,)),
            dma((devices,)),
            dma((devices,)),
            dma,
            dma,
        ],
        compiler_params=pltpu.CompilerParams(
            collective_id=0, has_side_effects=True, vmem_limit_bytes=60 * 1024 * 1024
        ),
        cost_estimate=pl.CostEstimate(flops=flops, bytes_accessed=2 * out_weight.size, transcendentals=0),
        name="layer",
    )(first.reshape(1), table, packed, query_parts, out_weight)


def local(query_states, key_states, value_rows, positions, out_weight):
    tokens, query_heads, head_size = query_states.shape
    kv_heads = key_states.shape[1]
    group = query_heads // kv_heads
    half = tokens // 2
    devices = lax.axis_size("ctx")
    blocks = 2 * devices
    parts = lax.axis_size("groups")
    me_part = lax.axis_index("groups")
    share = out_weight.shape[1] // parts
    query_parts = query_states.reshape(2, half, kv_heads, group, head_size).transpose(2, 0, 3, 1, 4)
    query_parts = query_parts.reshape(kv_heads, 2, group * half, head_size)
    if parts == 2 and lax.axis_size("tp") == 1 and devices == 4 * BLOCKS_PER_STEP and share % 128 == 0:
        packed = jnp.concatenate(
            [key_states.reshape(tokens, kv_heads * head_size), value_rows.reshape(tokens, kv_heads * head_size)], axis=1
        )
        return layer(query_parts, packed, positions[0] // half, out_weight, half)
    weight_share = lax.dynamic_slice_in_dim(out_weight, me_part * share, share, 1)
    weight = lax.all_gather(weight_share, "ctx", axis=1, tiled=True)
    packed = jnp.concatenate(
        [key_states.reshape(tokens, kv_heads * head_size), value_rows.reshape(tokens, kv_heads * head_size)], axis=1
    )
    first = positions[0] // half
    tail = jnp.broadcast_to(first.astype(packed.dtype), (TAIL, packed.shape[1]))
    gathered = spread(jnp.concatenate([packed, tail], axis=0))
    firsts = gathered[:, tokens, 0].astype(jnp.int32)
    gathered = gathered.reshape(devices * (tokens + TAIL), packed.shape[1])
    wanted = jnp.arange(blocks, dtype=jnp.int32)[:, None]
    stored = jnp.stack([firsts, blocks - 1 - firsts], axis=1).reshape(1, blocks)
    kept = jnp.arange(blocks, dtype=jnp.int32)[None, :]
    starts = kept // 2 * (tokens + TAIL) + kept % 2 * half
    place = jnp.sum(jnp.where(stored == wanted, starts, 0), axis=1)
    place = place.astype(jnp.int32)
    own = jnp.stack([first, blocks - 1 - first]).astype(jnp.int32)
    pieces = min(2, kv_heads)
    span = kv_heads // pieces
    attended = [
        attend(query_parts[i * span : (i + 1) * span], gathered, place, own, i * span, kv_heads, half) for i in range(pieces)
    ]

    def project(rows):
        product = lax.dot_general(
            jnp.concatenate(rows, axis=0), weight, (((0,), (0,)), ((), ())), preferred_element_type=jnp.float32
        )
        return product.astype(jnp.bfloat16)

    guests = [[hand_on(piece, by) for piece in attended] for by in range(1, parts)]
    mine = project(attended)
    results = [mine] + [hand_on(project(rows), parts - 1 - i) for i, rows in enumerate(guests)]
    if share % 128 == 0:
        combined = weave(results, me_part, devices)
    else:
        shares = jnp.stack([r.reshape(tokens, devices, share) for r in results])
        order = (jnp.arange(parts) - me_part) % parts
        combined = jnp.moveaxis(jnp.take(shares, order, axis=0), 0, 2).reshape(tokens, devices * parts * share)
    return lax.psum_scatter(combined, "tp", scatter_dimension=1, tiled=True)


def solution(mesh):
    in_specs = (
        P(("groups", "ctx"), "tp", None),
        P(("groups", "ctx"), "tp", None),
        P(("groups", "ctx"), "tp", None),
        P(("groups", "ctx")),
        P("tp", "ctx"),
    )
    out_specs = P(("groups", "ctx"), "tp")
    return jax.shard_map(local, mesh=mesh, in_specs=in_specs, out_specs=out_specs, check_vma=False)
```

```python
import functools
import math

import jax
import jax.numpy as jnp
from jax import lax
from jax.experimental import pallas as pl
from jax.experimental.pallas import tpu as pltpu
from jax.sharding import PartitionSpec as P

LOW_START = -1e30
BLOCKS_PER_STEP = 4
CHUNK = 1024
TAIL = 16
VMEM = 50 * 1024 * 1024


def attend_kernel(half, group, place_ref, own_ref, q_ref, k_ref, v_ref, out_ref, acc_ref, max_ref, sum_ref):
    rows = group * half
    head_size = q_ref.shape[-1]
    span = BLOCKS_PER_STEP * half
    chunk = min(CHUNK, rows)
    to_exp2 = head_size ** (-0.5) * math.log2(math.e)

    def step(which, number, masked, query_block):
        keys, values = [], []
        for i in range(BLOCKS_PER_STEP):
            place = place_ref[number * BLOCKS_PER_STEP + i]
            keys.append(k_ref[pl.ds(pl.multiple_of(place, TAIL), half), :])
            values.append(v_ref[pl.ds(pl.multiple_of(place, TAIL), half), :])
        key_part = jnp.concatenate(keys, axis=0)
        value_part = jnp.concatenate(values, axis=0)
        if masked:
            key_place = number * span + lax.broadcasted_iota(jnp.int32, (span, chunk), 0)
            query_place = query_block * half + lax.broadcasted_iota(jnp.int32, (span, chunk), 1) % half
            visible = key_place <= query_place
        for c in range(rows // chunk):
            cols = pl.ds(c * chunk, chunk)
            scores = lax.dot_general(
                key_part,
                q_ref[0, which, cols, :],
                (((1,), (1,)), ((), ())),
                preferred_element_type=jnp.float32,
            )
            if masked:
                scores = jnp.where(visible, scores, LOW_START)
            old_max = max_ref[:, cols]
            new_max = jnp.maximum(old_max, jnp.max(scores, axis=0, keepdims=True))
            factor = jnp.exp2((old_max - new_max) * to_exp2)
            exp_scores = jnp.exp2((scores - new_max) * to_exp2)
            max_ref[:, cols] = new_max
            sum_ref[:, cols] = sum_ref[:, cols] * factor + jnp.sum(exp_scores, axis=0, keepdims=True)
            weighted = lax.dot_general(
                value_part,
                exp_scores.astype(jnp.bfloat16),
                (((0,), (0,)), ((), ())),
                preferred_element_type=jnp.float32,
            )
            acc_ref[:, cols] = acc_ref[:, cols] * factor + weighted

    for which in range(2):
        query_block = own_ref[which]
        steps = query_block // BLOCKS_PER_STEP
        max_ref[...] = jnp.full_like(max_ref, LOW_START)
        sum_ref[...] = jnp.zeros_like(sum_ref)
        acc_ref[...] = jnp.zeros_like(acc_ref)

        @pl.loop(0, steps)
        def _(number):
            step(which, number, False, query_block)

        step(which, steps, True, query_block)
        for g in range(group):
            cols = pl.ds(g * half, half)
            attended = acc_ref[:, cols] / sum_ref[:, cols]
            out_ref[pl.ds(g * head_size, head_size), pl.ds(which * half, half)] = attended.astype(jnp.bfloat16)


def attend(query_parts, gathered, place, own, first_head, all_heads, half):
    kv_heads, _, rows, head_size = query_parts.shape
    keys_total = gathered.shape[0]
    blocks = place.shape[0]
    group = rows // half
    flops = 4 * kv_heads * rows * head_size * half * (blocks + 1)
    return pl.pallas_call(
        functools.partial(attend_kernel, half, group),
        out_shape=jax.ShapeDtypeStruct((kv_heads * group * head_size, 2 * half), jnp.bfloat16),
        grid_spec=pltpu.PrefetchScalarGridSpec(
            num_scalar_prefetch=2,
            grid=(kv_heads,),
            in_specs=[
                pl.BlockSpec((1, 2, rows, head_size), lambda h, *_: (h, 0, 0, 0)),
                pl.BlockSpec((keys_total, head_size), lambda h, *_: (0, h + first_head)),
                pl.BlockSpec((keys_total, head_size), lambda h, *_: (0, h + first_head + all_heads)),
            ],
            out_specs=pl.BlockSpec((group * head_size, 2 * half), lambda h, *_: (h, 0)),
            scratch_shapes=[
                pltpu.VMEM((head_size, rows), jnp.float32),
                pltpu.VMEM((1, rows), jnp.float32),
                pltpu.VMEM((1, rows), jnp.float32),
            ],
        ),
        compiler_params=pltpu.CompilerParams(
            dimension_semantics=("arbitrary",), vmem_limit_bytes=20 * 1024 * 1024
        ),
        cost_estimate=pl.CostEstimate(
            flops=flops, bytes_accessed=2 * gathered.size, transcendentals=flops // (4 * head_size)
        ),
        name="attend",
    )(place, own, query_parts, gathered, gathered)


def spread_kernel(devices, own_ref, out_ref, far_send, far_recv, side_send, side_recv, pair_send, pair_recv, own_sem):
    me = lax.axis_index("ctx")
    outers = devices // 4
    outer, middle, inner = me // 4, (me // 2) % 2, me % 2

    def at(o, m, i):
        return (o * 2 + m) * 2 + i

    side = at(outer, 1 - middle, inner)
    pair = at(outer, middle, 1 - inner)
    far = [at((outer + k) % outers, middle, inner) for k in range(1, outers)]
    barrier = pltpu.get_barrier_semaphore()
    for other in far + [side, pair]:
        pl.semaphore_signal(barrier, inc=1, device_id={"ctx": other}, device_id_type=pl.DeviceIdType.MESH)
    pl.semaphore_wait(barrier, outers + 1)

    def send(source, slot, sends, recvs, number, target):
        return pltpu.make_async_remote_copy(
            src_ref=source,
            dst_ref=out_ref.at[slot],
            send_sem=sends.at[number],
            recv_sem=recvs.at[number],
            device_id={"ctx": target},
            device_id_type=pl.DeviceIdType.MESH,
        )

    own = pltpu.make_async_copy(own_ref, out_ref.at[me], own_sem)
    far_copies = [send(own_ref, me, far_send, far_recv, k, far[k]) for k in range(outers - 1)]
    for copy in far_copies:
        copy.start()
    side_copies = [send(own_ref, me, side_send, side_recv, 0, side)]
    pair_copies = [send(own_ref, me, pair_send, pair_recv, 0, pair)]
    side_copies[0].start()
    pair_copies[0].start()
    own.start()
    for k in range(outers - 1):
        far_copies[k].wait_recv()
        slot = at((outer + outers - 1 - k) % outers, middle, inner)
        side_copies.append(send(out_ref.at[slot], slot, side_send, side_recv, k + 1, side))
        pair_copies.append(send(out_ref.at[slot], slot, pair_send, pair_recv, k + 1, pair))
        side_copies[-1].start()
        pair_copies[-1].start()
    for k in range(outers):
        side_copies[k].wait_recv()
        slot = at((outer + outers - k) % outers, 1 - middle, inner)
        pair_copies.append(send(out_ref.at[slot], slot, pair_send, pair_recv, outers + k, pair))
        pair_copies[-1].start()
    for copy in pair_copies:
        copy.wait_recv()
    for copy in far_copies + side_copies + pair_copies:
        copy.wait_send()
    own.wait()


def spread(packed):
    devices = lax.axis_size("ctx")
    outers = devices // 4
    rows, columns = packed.shape
    gathered = pl.pallas_call(
        functools.partial(spread_kernel, devices),
        out_shape=jax.ShapeDtypeStruct((devices, rows, columns), packed.dtype),
        in_specs=[pl.BlockSpec(memory_space=pltpu.VMEM)],
        out_specs=pl.BlockSpec(memory_space=pltpu.VMEM),
        scratch_shapes=[
            pltpu.SemaphoreType.DMA((outers - 1,)),
            pltpu.SemaphoreType.DMA((outers - 1,)),
            pltpu.SemaphoreType.DMA((outers,)),
            pltpu.SemaphoreType.DMA((outers,)),
            pltpu.SemaphoreType.DMA((2 * outers,)),
            pltpu.SemaphoreType.DMA((2 * outers,)),
            pltpu.SemaphoreType.DMA,
        ],
        compiler_params=pltpu.CompilerParams(
            collective_id=0, has_side_effects=True, vmem_limit_bytes=24 * 1024 * 1024
        ),
        cost_estimate=pl.CostEstimate(flops=0, bytes_accessed=20 * packed.size * devices, transcendentals=0),
        name="spread",
    )(packed)
    return gathered


def hand_on(value, by):
    parts = lax.axis_size("groups")
    return lax.ppermute(value, "groups", [(i, (i + by) % parts) for i in range(parts)])


def weave_kernel(share, me_ref, *refs):
    *shares, out_ref = refs
    parts = len(shares)
    for p in range(parts):
        by = lax.rem(p - me_ref[0] + parts, parts)
        chosen = shares[0][...]
        for k in range(1, parts):
            chosen = jnp.where(by == k, shares[k][...], chosen)
        for i in range(chosen.shape[1] // share):
            out_ref[:, (i * parts + p) * share : (i * parts + p + 1) * share] = chosen[:, i * share : (i + 1) * share]


def weave(results, me_part, devices):
    parts = len(results)
    tokens, columns = results[0].shape
    share = columns // devices
    return pl.pallas_call(
        functools.partial(weave_kernel, share),
        out_shape=jax.ShapeDtypeStruct((tokens, parts * columns), results[0].dtype),
        grid_spec=pltpu.PrefetchScalarGridSpec(
            num_scalar_prefetch=1,
            grid=(devices // 4,),
            in_specs=[pl.BlockSpec((tokens, 4 * share), lambda i, *_: (0, i))] * parts,
            out_specs=pl.BlockSpec((tokens, 4 * parts * share), lambda i, *_: (0, i)),
        ),
        name="weave",
    )(me_part.astype(jnp.int32).reshape(1), *results)


def layer_kernel(sizes, first_ref, table_ref, kv_ref, q_ref, w_ref, out_ref, *scratch):
    devices, half, kv_heads, group, head_size, share = sizes
    (kv_low, kv_high, firsts, place_vec, place_ref, w_all, acc_ref, max_ref, sum_ref, rows_ref, back_ref, *sems) = scratch
    (far_send, far_recv, side_send, side_recv, pair_send, pair_recv) = sems[:6]
    (wfar_send, wfar_recv, wside_send, wside_recv, wpair_send, wpair_recv) = sems[6:12]
    (rows_send, rows_recv, back_send, back_recv, pass_send, wpass_send, own_sem, place_sem) = sems[12:]
    outers = devices // 4
    blocks = 2 * devices
    tokens = 2 * half
    width = group * half
    depth = kv_heads * group * head_size
    pieces = kv_heads
    piece = depth // pieces
    span = BLOCKS_PER_STEP * half
    groups = devices // BLOCKS_PER_STEP
    to_exp2 = head_size ** (-0.5) * math.log2(math.e)

    part = lax.axis_index("groups")
    me = lax.axis_index("ctx")
    outer, middle, inner = me // 4, (me // 2) % 2, me % 2

    def flip(number, by):
        result, unit = 0, 1
        while unit < outers:
            result = result + (number // unit + by // unit) % 2 * unit
            unit *= 2
        return result

    def slot_of(hop, cross, swap):
        return (flip(outer, hop) * 2 + (middle + cross) % 2) * 2 + (inner + swap) % 2

    far = [slot_of(k, 0, 0) for k in range(outers)]
    side = slot_of(0, 1, 0)
    pair = slot_of(0, 0, 1)
    inside = jnp.logical_and(outer > 0, outer < outers - 1)
    last = pieces - 1
    guest = lax.rem(part + 1, 2)

    barrier = pltpu.get_barrier_semaphore()
    for other in far[1:] + [side, pair]:
        pl.semaphore_signal(barrier, inc=1, device_id={"ctx": other}, device_id_type=pl.DeviceIdType.MESH)
    pl.semaphore_signal(barrier, inc=1, device_id={"groups": guest}, device_id_type=pl.DeviceIdType.MESH)
    pl.semaphore_wait(barrier, outers + 2)

    def remote(source, target, send, recv, axis, index):
        return pltpu.make_async_remote_copy(
            src_ref=source,
            dst_ref=target,
            send_sem=send,
            recv_sem=recv,
            device_id={axis: index},
            device_id_type=pl.DeviceIdType.MESH,
        )

    def own_item(item):
        return table_ref if item == 0 else kv_ref.at[pl.ds((item - 1) * half, half), :]

    def item_at(item, slot):
        if item == 0:
            return firsts.at[slot]
        return (kv_low if item == 1 else kv_high).at[slot]

    def source_of(item, hop, cross):
        return own_item(item) if hop == 0 and cross == 0 else item_at(item, slot_of(hop, cross, 0))

    def far_copy(item, hop):
        return remote(own_item(item), item_at(item, me), far_send.at[item, hop], far_recv.at[item, hop], "ctx", far[hop])

    def pass_copy(item):
        ref = item_at(item, far[2])
        return remote(ref, ref, pass_send.at[item], far_recv.at[item, 3], "ctx", far[1])

    def side_copy(item, hop):
        return remote(
            source_of(item, hop, 0), item_at(item, far[hop]), side_send.at[item, hop], side_recv.at[item, hop], "ctx", side
        )

    def pair_copy(item, hop, cross):
        n = hop * 2 + cross
        return remote(
            source_of(item, hop, cross),
            item_at(item, slot_of(hop, cross, 0)),
            pair_send.at[item, n],
            pair_recv.at[item, n],
            "ctx",
            pair,
        )

    def w_at(slot, n):
        return w_all.at[slot, pl.ds(n * piece, piece), :]

    def far_part(hop, e):
        return w_at(slot_of(hop, 0, 0), e) if e < pieces else w_at(slot_of(hop, 1, 0), last)

    def wfar_copy(hop, e):
        ref = far_part(0, e)
        return remote(ref, ref, wfar_send.at[hop, e], wfar_recv.at[hop, e], "ctx", far[hop])

    def wpass_copy(e):
        ref = far_part(2, e)
        return remote(ref, ref, wpass_send.at[e], wfar_recv.at[3, e], "ctx", far[1])

    def wside_copy(hop, n):
        ref = w_at(far[hop], n)
        return remote(ref, ref, wside_send.at[hop, n], wside_recv.at[hop, n], "ctx", side)

    def wpair_copy(hop, cross, n):
        ref = w_at(slot_of(hop, cross, 0), n)
        return remote(ref, ref, wpair_send.at[hop * 2 + cross, n], wpair_recv.at[hop * 2 + cross, n], "ctx", pair)

    def rows_copy(which, h):
        cols = pl.ds(pl.multiple_of(h * piece, piece), piece)
        return remote(
            rows_ref.at[pl.ds(which * half, half), cols],
            rows_ref.at[pl.ds(tokens + which * half, half), cols],
            rows_send.at[which, h],
            rows_recv.at[which, h],
            "groups",
            guest,
        )

    def back_copy(n, slot):
        cols = pl.ds(pl.multiple_of((slot * 2 + part) * share, share), share)
        return remote(back_ref.at[n], out_ref.at[:, cols], back_send.at[n], back_recv.at[n], "groups", guest)

    def far_start(copy, hop):
        if hop == 3:

            @pl.when(inside)
            def _():
                copy.start()

        else:
            copy.start()

    def pass_on(copy):
        @pl.when(inside)
        def _():
            copy.start()

    def far_arrived(item, hop):
        far_copy(item, hop).wait_recv()
        if hop == 2:
            pass_on(pass_copy(item))
        side_copy(item, hop).start()
        pair_copy(item, hop, 0).start()

    def side_arrived(item, hop):
        side_copy(item, hop).wait_recv()
        pair_copy(item, hop, 1).start()

    def pair_arrived(item, hop):
        for cross in range(2):
            pair_copy(item, hop, cross).wait_recv()

    def wfar_arrived(hop, e):
        wfar_copy(hop, e).wait_recv()
        if hop == 2:
            pass_on(wpass_copy(e))
        if e < last:
            wside_copy(hop, e).start()
        wpair_copy(hop, 1 if e == pieces else 0, min(e, last)).start()

    def wside_arrived(hop, n):
        wside_copy(hop, n).wait_recv()
        wpair_copy(hop, 1, n).start()

    own_weight = pltpu.make_async_copy(
        w_ref.at[:, pl.ds(pl.multiple_of(part * share, share), share)], w_all.at[me], own_sem
    )
    own_weight.start()
    def own_start(item):
        for hop in range(1, outers):
            far_start(far_copy(item, hop), hop)

    for item in range(2):
        side_copy(item, 0).start()
        own_start(item)
        pair_copy(item, 0, 0).start()
    pair_copy(2, 0, 0).start()
    kv_low[me] = kv_ref[:half, :]
    kv_high[me] = kv_ref[half:, :]
    firsts[me] = table_ref[...]

    def clear(at):
        max_ref[at] = jnp.full(max_ref.shape[1:], LOW_START, jnp.float32)
        sum_ref[at] = jnp.zeros(sum_ref.shape[1:], jnp.float32)
        acc_ref[at] = jnp.zeros(acc_ref.shape[1:], jnp.float32)

    for h in range(kv_heads):
        clear(h)
    own_weight.wait()

    def step(h, which, source, places, at, visible):
        keys = pl.ds(pl.multiple_of(h * head_size, head_size), head_size)
        values = pl.ds(pl.multiple_of((kv_heads + h) * head_size, head_size), head_size)
        key_part = jnp.concatenate([source[p, :, keys] for p in places], axis=0)
        value_part = jnp.concatenate([source[p, :, values] for p in places], axis=0)
        scores = lax.dot_general(
            key_part, q_ref[h, which], (((1,), (1,)), ((), ())), preferred_element_type=jnp.float32
        )
        old_max = max_ref[at]
        if visible is not None:
            scores = jnp.where(visible, scores, LOW_START)
        new_max = jnp.maximum(old_max, jnp.max(scores, axis=0, keepdims=True))
        factor = jnp.exp2((old_max - new_max) * to_exp2)
        exp_scores = jnp.exp2((scores - new_max) * to_exp2)
        max_ref[at] = new_max
        sum_ref[at] = sum_ref[at] * factor + jnp.sum(exp_scores, axis=0, keepdims=True)
        weighted = lax.dot_general(
            value_part,
            exp_scores.astype(jnp.bfloat16),
            (((0,), (0,)), ((), ())),
            preferred_element_type=jnp.float32,
        )
        acc_ref[at] = acc_ref[at] * factor + weighted

    def run_hooks(number, hooks):
        for at, actions in hooks.items():

            @pl.when(number == at)
            def _():
                for action in actions:
                    action()

    def low_blocks(hop, hooks):
        start = flip(outer, hop) * 4

        @pl.loop(0, kv_heads)
        def _(h):
            run_hooks(h, hooks)
            step(h, 1, kv_low, [start + i for i in range(4)], h, None)

    def low_side(hop):
        for item in range(2):
            side_arrived(item, hop)

    def low_far(hop):
        for item in range(2):
            far_arrived(item, hop)

    def low_pair(hop):
        for item in range(2):
            pair_arrived(item, hop)

    def weight_round(e):
        for hop in (2, 1, 3):
            far_start(wfar_copy(hop, e), hop)

    def weight_own(n):
        wside_copy(0, n).start()
        wpair_copy(0, 0, n).start()

    def do(action, *args):
        return functools.partial(action, *args)

    low_side(0)
    low_pair(0)
    low_blocks(0, {2: [do(low_far, 1)], 3: [do(own_start, 2)]})
    low_far(2)
    low_side(1)
    low_pair(1)
    low_blocks(1, {0: [side_copy(2, 0).start], 2: [do(low_far, 3)]})
    low_side(2)
    low_pair(2)
    low_blocks(2, {1: [do(far_arrived, 2, 1)], 3: [do(far_arrived, 2, 2), do(weight_round, 0)]})
    low_side(3)
    low_pair(3)
    lanes = lax.broadcasted_iota(jnp.int32, firsts.shape[1:], 1)
    numbers = jnp.zeros(firsts.shape[1:], jnp.int32)
    for d in range(devices):
        numbers = numbers + jnp.where(firsts[d] == lanes, d, 0)
        numbers = numbers + jnp.where(blocks - 1 - firsts[d] == lanes, d, 0)
    place_vec[...] = jnp.minimum(numbers, devices - 1)
    low_blocks(3, {0: [do(side_arrived, 2, 0)], 1: [do(weight_own, last)], 3: [do(far_arrived, 2, 3)]})
    to_scalars = pltpu.make_async_copy(place_vec, place_ref, place_sem)
    to_scalars.start()
    to_scalars.wait()

    first = first_ref[0]
    key_rows = lax.broadcasted_iota(jnp.int32, (span, width), 0)
    query_cols = lax.broadcasted_iota(jnp.int32, (span, width), 1) % half

    def finish(which, hooks):
        block = blocks - 1 - first if which else first

        @pl.loop(0, kv_heads)
        def _(h):
            at = h if which else kv_heads
            if not which:
                clear(at)

            @pl.loop(0, groups)
            def _(t):
                run_hooks(h * groups + t, hooks)

                @pl.when(jnp.logical_and(t == 1, h > 0))
                def _():
                    rows_copy(which, h - 1).start()

                number = groups + t if which else t
                places = [place_ref[0, number * BLOCKS_PER_STEP + i] for i in range(BLOCKS_PER_STEP)]
                visible = number * span + key_rows <= block * half + query_cols
                step(h, which, kv_high if which else kv_low, places, at, visible)

            for g in range(group):
                cols = pl.ds(g * half, half)
                attended = acc_ref[at, :, cols] / sum_ref[at, :, cols]
                target = pl.ds(pl.multiple_of(h * piece + g * head_size, head_size), head_size)
                rows_ref[pl.ds(which * half, half), target] = attended.T.astype(jnp.bfloat16)

    finish(
        0,
        {
            0: [do(side_arrived, 2, 1), do(weight_own, 0)],
            1: [do(weight_round, 1)],
            4: [do(side_arrived, 2, 2)],
            5: [do(weight_own, 1)],
            8: [do(side_arrived, 2, 3), do(weight_own, 2)],
            10: [do(wfar_arrived, 1, 0)],
            11: [do(wfar_arrived, 2, 0)],
            12: [do(weight_round, 2)],
        },
    )
    for hop in range(outers):
        pair_arrived(2, hop)
    rows_copy(0, kv_heads - 1).start()
    finish(
        1,
        {
            1: [do(wside_arrived, 0, last)],
            2: [do(wfar_arrived, 3, 0)],
            3: [do(weight_round, last)],
            4: [do(wfar_arrived, 1, 1)],
            5: [do(wside_arrived, 0, 0)],
            7: [do(wfar_arrived, 2, 1)],
            9: [do(wside_arrived, 0, 1)],
            11: [do(weight_round, pieces)],
            12: [do(wfar_arrived, 1, 2)],
            13: [do(wfar_arrived, 3, 1)],
            14: [do(wside_arrived, 0, 2)],
            15: [do(wfar_arrived, 2, 2), do(wside_arrived, 1, 0)],
        },
    )
    wside_arrived(2, 0)
    rows_copy(1, kv_heads - 1).start()

    def project(hop, cross):
        n = hop * 2 + cross
        base = slot_of(hop, cross, 0) - inner
        for m in range(pieces):
            wpair_copy(hop, cross, m).wait_recv()
        weight = jnp.concatenate([w_all[base], w_all[base + 1]], axis=1)
        product = lax.dot_general(
            rows_ref[...], weight, (((1,), (0,)), ((), ())), preferred_element_type=jnp.float32
        ).astype(jnp.bfloat16)
        for i in range(2):
            back_ref[n * 2 + i] = product[tokens:, i * share : (i + 1) * share]
        for i in range(2):
            cols = pl.ds(pl.multiple_of(((base + i) * 2 + part) * share, share), share)
            out_ref[:, cols] = product[:tokens, i * share : (i + 1) * share]
        for i in range(2):
            back_copy(n * 2 + i, base + i).start()

    wfar_arrived(3, 2)
    wside_arrived(3, 0)
    for which in range(2):
        for h in range(kv_heads):
            rows_copy(which, h).wait_recv()
    wside_arrived(1, 1)
    project(0, 0)
    wfar_arrived(1, last)
    wfar_arrived(2, last)
    project(0, 1)
    wside_arrived(2, 1)
    wfar_arrived(1, pieces)
    wfar_arrived(2, pieces)
    wside_arrived(3, 1)
    project(1, 0)
    wside_arrived(1, 2)
    project(1, 1)
    wfar_arrived(3, last)
    project(2, 0)
    wside_arrived(2, 2)
    project(2, 1)
    wfar_arrived(3, pieces)
    project(3, 0)
    wside_arrived(3, 2)
    project(3, 1)

    for n in range(2 * 2 * outers):
        back_copy(n, 0).wait_recv()
    for n in range(2 * 2 * outers):
        back_copy(n, 0).wait_send()
    for which in range(2):
        for h in range(kv_heads):
            rows_copy(which, h).wait_send()
    for hop in range(outers):
        for item in range(3):
            if 0 < hop < 3:
                far_copy(item, hop).wait_send()
            side_copy(item, hop).wait_send()
            for cross in range(2):
                pair_copy(item, hop, cross).wait_send()
        for n in range(pieces):
            if hop == 0 or n < last:
                wside_copy(hop, n).wait_send()
            for cross in range(2):
                wpair_copy(hop, cross, n).wait_send()
        for e in range(pieces + 1):
            if 0 < hop < 3:
                wfar_copy(hop, e).wait_send()

    @pl.when(inside)
    def _():
        for item in range(3):
            far_copy(item, 3).wait_send()
            pass_copy(item).wait_send()
        for e in range(pieces + 1):
            wfar_copy(3, e).wait_send()
            wpass_copy(e).wait_send()


def layer(query_parts, packed, first, out_weight, half):
    devices = lax.axis_size("ctx")
    outers = devices // 4
    kv_heads, _, width, head_size = query_parts.shape
    group = width // half
    tokens = 2 * half
    depth, columns = out_weight.shape
    share = columns // 2
    slots = kv_heads + 1
    pieces = kv_heads
    table = jnp.full((8, 128), first, jnp.int32)
    dma = pltpu.SemaphoreType.DMA
    flops = 4 * query_parts.size * half * (2 * devices + 1) // 2 + 4 * tokens * depth * columns * devices // 2
    return pl.pallas_call(
        functools.partial(layer_kernel, (devices, half, kv_heads, group, head_size, share)),
        out_shape=jax.ShapeDtypeStruct((tokens, columns * devices), jnp.bfloat16),
        in_specs=[
            pl.BlockSpec(memory_space=pltpu.SMEM),
            pl.BlockSpec(memory_space=pltpu.VMEM),
            pl.BlockSpec(memory_space=pltpu.VMEM),
            pl.BlockSpec(memory_space=pltpu.VMEM),
            pl.BlockSpec(memory_space=pl.ANY),
        ],
        out_specs=pl.BlockSpec(memory_space=pltpu.VMEM),
        scratch_shapes=[
            pltpu.VMEM((devices, half, packed.shape[1]), packed.dtype),
            pltpu.VMEM((devices, half, packed.shape[1]), packed.dtype),
            pltpu.VMEM((devices, 8, 128), jnp.int32),
            pltpu.VMEM((8, 128), jnp.int32),
            pltpu.SMEM((8, 128), jnp.int32),
            pltpu.VMEM((devices, depth, share), out_weight.dtype),
            pltpu.VMEM((slots, head_size, width), jnp.float32),
            pltpu.VMEM((slots, 1, width), jnp.float32),
            pltpu.VMEM((slots, 1, width), jnp.float32),
            pltpu.VMEM((2 * tokens, depth), jnp.bfloat16),
            pltpu.VMEM((devices, tokens, share), jnp.bfloat16),
            dma((3, outers)),
            dma((3, outers)),
            dma((3, outers)),
            dma((3, outers)),
            dma((3, 2 * outers)),
            dma((3, 2 * outers)),
            dma((outers, pieces + 1)),
            dma((outers, pieces + 1)),
            dma((outers, pieces)),
            dma((outers, pieces)),
            dma((2 * outers, pieces)),
            dma((2 * outers, pieces)),
            dma((2, kv_heads)),
            dma((2, kv_heads)),
            dma((devices,)),
            dma((devices,)),
            dma((3,)),
            dma((pieces + 1,)),
            dma,
            dma,
        ],
        compiler_params=pltpu.CompilerParams(
            collective_id=0, has_side_effects=True, vmem_limit_bytes=VMEM
        ),
        cost_estimate=pl.CostEstimate(flops=flops, bytes_accessed=2 * out_weight.size, transcendentals=0),
        name="layer",
    )(first.reshape(1), table, packed, query_parts, out_weight)


def local(query_states, key_states, value_rows, positions, out_weight):
    tokens, query_heads, head_size = query_states.shape
    kv_heads = key_states.shape[1]
    group = query_heads // kv_heads
    half = tokens // 2
    devices = lax.axis_size("ctx")
    blocks = 2 * devices
    parts = lax.axis_size("groups")
    me_part = lax.axis_index("groups")
    share = out_weight.shape[1] // parts
    query_parts = query_states.reshape(2, half, kv_heads, group, head_size).transpose(2, 0, 3, 1, 4)
    query_parts = query_parts.reshape(kv_heads, 2, group * half, head_size)
    if parts == 2 and lax.axis_size("tp") == 1 and devices == 4 * BLOCKS_PER_STEP and share % 128 == 0:
        packed = jnp.concatenate(
            [key_states.reshape(tokens, kv_heads * head_size), value_rows.reshape(tokens, kv_heads * head_size)], axis=1
        )
        return layer(query_parts, packed, positions[0] // half, out_weight, half)
    weight_share = lax.dynamic_slice_in_dim(out_weight, me_part * share, share, 1)
    weight = lax.all_gather(weight_share, "ctx", axis=1, tiled=True)
    packed = jnp.concatenate(
        [key_states.reshape(tokens, kv_heads * head_size), value_rows.reshape(tokens, kv_heads * head_size)], axis=1
    )
    first = positions[0] // half
    tail = jnp.broadcast_to(first.astype(packed.dtype), (TAIL, packed.shape[1]))
    gathered = spread(jnp.concatenate([packed, tail], axis=0))
    firsts = gathered[:, tokens, 0].astype(jnp.int32)
    gathered = gathered.reshape(devices * (tokens + TAIL), packed.shape[1])
    wanted = jnp.arange(blocks, dtype=jnp.int32)[:, None]
    stored = jnp.stack([firsts, blocks - 1 - firsts], axis=1).reshape(1, blocks)
    kept = jnp.arange(blocks, dtype=jnp.int32)[None, :]
    starts = kept // 2 * (tokens + TAIL) + kept % 2 * half
    place = jnp.sum(jnp.where(stored == wanted, starts, 0), axis=1)
    place = place.astype(jnp.int32)
    own = jnp.stack([first, blocks - 1 - first]).astype(jnp.int32)
    pieces = min(2, kv_heads)
    span = kv_heads // pieces
    attended = [
        attend(query_parts[i * span : (i + 1) * span], gathered, place, own, i * span, kv_heads, half) for i in range(pieces)
    ]

    def project(rows):
        product = lax.dot_general(
            jnp.concatenate(rows, axis=0), weight, (((0,), (0,)), ((), ())), preferred_element_type=jnp.float32
        )
        return product.astype(jnp.bfloat16)

    guests = [[hand_on(piece, by) for piece in attended] for by in range(1, parts)]
    mine = project(attended)
    results = [mine] + [hand_on(project(rows), parts - 1 - i) for i, rows in enumerate(guests)]
    if share % 128 == 0:
        combined = weave(results, me_part, devices)
    else:
        shares = jnp.stack([r.reshape(tokens, devices, share) for r in results])
        order = (jnp.arange(parts) - me_part) % parts
        combined = jnp.moveaxis(jnp.take(shares, order, axis=0), 0, 2).reshape(tokens, devices * parts * share)
    return lax.psum_scatter(combined, "tp", scatter_dimension=1, tiled=True)


def solution(mesh):
    in_specs = (
        P(("groups", "ctx"), "tp", None),
        P(("groups", "ctx"), "tp", None),
        P(("groups", "ctx"), "tp", None),
        P(("groups", "ctx")),
        P("tp", "ctx"),
    )
    out_specs = P(("groups", "ctx"), "tp")
    return jax.shard_map(local, mesh=mesh, in_specs=in_specs, out_specs=out_specs, check_vma=False)
```

```python
import functools
import math

import jax
import jax.numpy as jnp
from jax import lax
from jax.experimental import pallas as pl
from jax.experimental.pallas import tpu as pltpu
from jax.sharding import PartitionSpec as P

LOW_START = -1e30
BLOCKS_PER_STEP = 4
CHUNK = 1024
TAIL = 16
VMEM = 50 * 1024 * 1024


def attend_kernel(half, group, place_ref, own_ref, q_ref, k_ref, v_ref, out_ref, acc_ref, max_ref, sum_ref):
    rows = group * half
    head_size = q_ref.shape[-1]
    span = BLOCKS_PER_STEP * half
    chunk = min(CHUNK, rows)
    to_exp2 = head_size ** (-0.5) * math.log2(math.e)

    def step(which, number, masked, query_block):
        keys, values = [], []
        for i in range(BLOCKS_PER_STEP):
            place = place_ref[number * BLOCKS_PER_STEP + i]
            keys.append(k_ref[pl.ds(pl.multiple_of(place, TAIL), half), :])
            values.append(v_ref[pl.ds(pl.multiple_of(place, TAIL), half), :])
        key_part = jnp.concatenate(keys, axis=0)
        value_part = jnp.concatenate(values, axis=0)
        if masked:
            key_place = number * span + lax.broadcasted_iota(jnp.int32, (span, chunk), 0)
            query_place = query_block * half + lax.broadcasted_iota(jnp.int32, (span, chunk), 1) % half
            visible = key_place <= query_place
        for c in range(rows // chunk):
            cols = pl.ds(c * chunk, chunk)
            scores = lax.dot_general(
                key_part,
                q_ref[0, which, cols, :],
                (((1,), (1,)), ((), ())),
                preferred_element_type=jnp.float32,
            )
            if masked:
                scores = jnp.where(visible, scores, LOW_START)
            old_max = max_ref[:, cols]
            new_max = jnp.maximum(old_max, jnp.max(scores, axis=0, keepdims=True))
            factor = jnp.exp2((old_max - new_max) * to_exp2)
            exp_scores = jnp.exp2((scores - new_max) * to_exp2)
            max_ref[:, cols] = new_max
            sum_ref[:, cols] = sum_ref[:, cols] * factor + jnp.sum(exp_scores, axis=0, keepdims=True)
            weighted = lax.dot_general(
                value_part,
                exp_scores.astype(jnp.bfloat16),
                (((0,), (0,)), ((), ())),
                preferred_element_type=jnp.float32,
            )
            acc_ref[:, cols] = acc_ref[:, cols] * factor + weighted

    for which in range(2):
        query_block = own_ref[which]
        steps = query_block // BLOCKS_PER_STEP
        max_ref[...] = jnp.full_like(max_ref, LOW_START)
        sum_ref[...] = jnp.zeros_like(sum_ref)
        acc_ref[...] = jnp.zeros_like(acc_ref)

        @pl.loop(0, steps)
        def _(number):
            step(which, number, False, query_block)

        step(which, steps, True, query_block)
        for g in range(group):
            cols = pl.ds(g * half, half)
            attended = acc_ref[:, cols] / sum_ref[:, cols]
            out_ref[pl.ds(g * head_size, head_size), pl.ds(which * half, half)] = attended.astype(jnp.bfloat16)


def attend(query_parts, gathered, place, own, first_head, all_heads, half):
    kv_heads, _, rows, head_size = query_parts.shape
    keys_total = gathered.shape[0]
    blocks = place.shape[0]
    group = rows // half
    flops = 4 * kv_heads * rows * head_size * half * (blocks + 1)
    return pl.pallas_call(
        functools.partial(attend_kernel, half, group),
        out_shape=jax.ShapeDtypeStruct((kv_heads * group * head_size, 2 * half), jnp.bfloat16),
        grid_spec=pltpu.PrefetchScalarGridSpec(
            num_scalar_prefetch=2,
            grid=(kv_heads,),
            in_specs=[
                pl.BlockSpec((1, 2, rows, head_size), lambda h, *_: (h, 0, 0, 0)),
                pl.BlockSpec((keys_total, head_size), lambda h, *_: (0, h + first_head)),
                pl.BlockSpec((keys_total, head_size), lambda h, *_: (0, h + first_head + all_heads)),
            ],
            out_specs=pl.BlockSpec((group * head_size, 2 * half), lambda h, *_: (h, 0)),
            scratch_shapes=[
                pltpu.VMEM((head_size, rows), jnp.float32),
                pltpu.VMEM((1, rows), jnp.float32),
                pltpu.VMEM((1, rows), jnp.float32),
            ],
        ),
        compiler_params=pltpu.CompilerParams(
            dimension_semantics=("arbitrary",), vmem_limit_bytes=20 * 1024 * 1024
        ),
        cost_estimate=pl.CostEstimate(
            flops=flops, bytes_accessed=2 * gathered.size, transcendentals=flops // (4 * head_size)
        ),
        name="attend",
    )(place, own, query_parts, gathered, gathered)


def spread_kernel(devices, own_ref, out_ref, far_send, far_recv, side_send, side_recv, pair_send, pair_recv, own_sem):
    me = lax.axis_index("ctx")
    outers = devices // 4
    outer, middle, inner = me // 4, (me // 2) % 2, me % 2

    def at(o, m, i):
        return (o * 2 + m) * 2 + i

    side = at(outer, 1 - middle, inner)
    pair = at(outer, middle, 1 - inner)
    far = [at((outer + k) % outers, middle, inner) for k in range(1, outers)]
    barrier = pltpu.get_barrier_semaphore()
    for other in far + [side, pair]:
        pl.semaphore_signal(barrier, inc=1, device_id={"ctx": other}, device_id_type=pl.DeviceIdType.MESH)
    pl.semaphore_wait(barrier, outers + 1)

    def send(source, slot, sends, recvs, number, target):
        return pltpu.make_async_remote_copy(
            src_ref=source,
            dst_ref=out_ref.at[slot],
            send_sem=sends.at[number],
            recv_sem=recvs.at[number],
            device_id={"ctx": target},
            device_id_type=pl.DeviceIdType.MESH,
        )

    own = pltpu.make_async_copy(own_ref, out_ref.at[me], own_sem)
    far_copies = [send(own_ref, me, far_send, far_recv, k, far[k]) for k in range(outers - 1)]
    for copy in far_copies:
        copy.start()
    side_copies = [send(own_ref, me, side_send, side_recv, 0, side)]
    pair_copies = [send(own_ref, me, pair_send, pair_recv, 0, pair)]
    side_copies[0].start()
    pair_copies[0].start()
    own.start()
    for k in range(outers - 1):
        far_copies[k].wait_recv()
        slot = at((outer + outers - 1 - k) % outers, middle, inner)
        side_copies.append(send(out_ref.at[slot], slot, side_send, side_recv, k + 1, side))
        pair_copies.append(send(out_ref.at[slot], slot, pair_send, pair_recv, k + 1, pair))
        side_copies[-1].start()
        pair_copies[-1].start()
    for k in range(outers):
        side_copies[k].wait_recv()
        slot = at((outer + outers - k) % outers, 1 - middle, inner)
        pair_copies.append(send(out_ref.at[slot], slot, pair_send, pair_recv, outers + k, pair))
        pair_copies[-1].start()
    for copy in pair_copies:
        copy.wait_recv()
    for copy in far_copies + side_copies + pair_copies:
        copy.wait_send()
    own.wait()


def spread(packed):
    devices = lax.axis_size("ctx")
    outers = devices // 4
    rows, columns = packed.shape
    gathered = pl.pallas_call(
        functools.partial(spread_kernel, devices),
        out_shape=jax.ShapeDtypeStruct((devices, rows, columns), packed.dtype),
        in_specs=[pl.BlockSpec(memory_space=pltpu.VMEM)],
        out_specs=pl.BlockSpec(memory_space=pltpu.VMEM),
        scratch_shapes=[
            pltpu.SemaphoreType.DMA((outers - 1,)),
            pltpu.SemaphoreType.DMA((outers - 1,)),
            pltpu.SemaphoreType.DMA((outers,)),
            pltpu.SemaphoreType.DMA((outers,)),
            pltpu.SemaphoreType.DMA((2 * outers,)),
            pltpu.SemaphoreType.DMA((2 * outers,)),
            pltpu.SemaphoreType.DMA,
        ],
        compiler_params=pltpu.CompilerParams(
            collective_id=0, has_side_effects=True, vmem_limit_bytes=24 * 1024 * 1024
        ),
        cost_estimate=pl.CostEstimate(flops=0, bytes_accessed=20 * packed.size * devices, transcendentals=0),
        name="spread",
    )(packed)
    return gathered


def hand_on(value, by):
    parts = lax.axis_size("groups")
    return lax.ppermute(value, "groups", [(i, (i + by) % parts) for i in range(parts)])


def weave_kernel(share, me_ref, *refs):
    *shares, out_ref = refs
    parts = len(shares)
    for p in range(parts):
        by = lax.rem(p - me_ref[0] + parts, parts)
        chosen = shares[0][...]
        for k in range(1, parts):
            chosen = jnp.where(by == k, shares[k][...], chosen)
        for i in range(chosen.shape[1] // share):
            out_ref[:, (i * parts + p) * share : (i * parts + p + 1) * share] = chosen[:, i * share : (i + 1) * share]


def weave(results, me_part, devices):
    parts = len(results)
    tokens, columns = results[0].shape
    share = columns // devices
    return pl.pallas_call(
        functools.partial(weave_kernel, share),
        out_shape=jax.ShapeDtypeStruct((tokens, parts * columns), results[0].dtype),
        grid_spec=pltpu.PrefetchScalarGridSpec(
            num_scalar_prefetch=1,
            grid=(devices // 4,),
            in_specs=[pl.BlockSpec((tokens, 4 * share), lambda i, *_: (0, i))] * parts,
            out_specs=pl.BlockSpec((tokens, 4 * parts * share), lambda i, *_: (0, i)),
        ),
        name="weave",
    )(me_part.astype(jnp.int32).reshape(1), *results)


def layer_kernel(sizes, order_ref, table_ref, kv_ref, q_raw, w_ref, out_ref, *scratch):
    devices, half, kv_heads, group, head_size, share = sizes
    (kv_low, kv_high, firsts, place_vec, place_ref, w_all, acc_ref, max_ref, sum_ref, rows_ref, back_ref, part_ref, q_in, q_ref, turn_ref, *sems) = scratch
    (far_send, far_recv, side_send, side_recv, pair_send, pair_recv) = sems[:6]
    (wfar_send, wfar_recv, wside_send, wside_recv, wpair_send, wpair_recv) = sems[6:12]
    (rows_send, rows_recv, back_send, back_recv, pass_send, wpass_send, own_sem, place_sem, q_sem) = sems[12:]
    outers = devices // 4
    blocks = 2 * devices
    tokens = 2 * half
    width = group * half
    depth = kv_heads * group * head_size
    pieces = kv_heads
    piece = depth // pieces
    span = BLOCKS_PER_STEP * half
    groups = devices // BLOCKS_PER_STEP
    to_exp2 = head_size ** (-0.5) * math.log2(math.e)

    part = lax.axis_index("groups")
    me = lax.axis_index("ctx")
    outer, middle, inner = me // 4, (me // 2) % 2, me % 2

    def flip(number, by):
        result, unit = 0, 1
        while unit < outers:
            result = result + (number // unit + by // unit) % 2 * unit
            unit *= 2
        return result

    def slot_of(hop, cross, swap):
        return (flip(outer, hop) * 2 + (middle + cross) % 2) * 2 + (inner + swap) % 2

    far = [slot_of(k, 0, 0) for k in range(outers)]
    side = slot_of(0, 1, 0)
    pair = slot_of(0, 0, 1)
    inside = jnp.logical_and(outer > 0, outer < outers - 1)
    last = pieces - 1
    guest = lax.rem(part + 1, 2)

    barrier = pltpu.get_barrier_semaphore()
    for other in far[1:] + [side, pair]:
        pl.semaphore_signal(barrier, inc=1, device_id={"ctx": other}, device_id_type=pl.DeviceIdType.MESH)
    pl.semaphore_signal(barrier, inc=1, device_id={"groups": guest}, device_id_type=pl.DeviceIdType.MESH)
    pl.semaphore_wait(barrier, outers + 2)

    def remote(source, target, send, recv, axis, index):
        return pltpu.make_async_remote_copy(
            src_ref=source,
            dst_ref=target,
            send_sem=send,
            recv_sem=recv,
            device_id={axis: index},
            device_id_type=pl.DeviceIdType.MESH,
        )

    def own_item(item):
        return table_ref if item == 0 else kv_ref.at[pl.ds((item - 1) * half, half), :]

    def item_at(item, slot):
        if item == 0:
            return firsts.at[slot]
        return (kv_low if item == 1 else kv_high).at[slot]

    def source_of(item, hop, cross):
        return own_item(item) if hop == 0 and cross == 0 else item_at(item, slot_of(hop, cross, 0))

    def far_copy(item, hop):
        return remote(own_item(item), item_at(item, me), far_send.at[item, hop], far_recv.at[item, hop], "ctx", far[hop])

    def pass_copy(item):
        ref = item_at(item, far[2])
        return remote(ref, ref, pass_send.at[item], far_recv.at[item, 3], "ctx", far[1])

    def side_copy(item, hop):
        return remote(
            source_of(item, hop, 0), item_at(item, far[hop]), side_send.at[item, hop], side_recv.at[item, hop], "ctx", side
        )

    def pair_copy(item, hop, cross):
        n = hop * 2 + cross
        return remote(
            source_of(item, hop, cross),
            item_at(item, slot_of(hop, cross, 0)),
            pair_send.at[item, n],
            pair_recv.at[item, n],
            "ctx",
            pair,
        )

    def w_at(slot, n):
        return w_all.at[slot, pl.ds(n * piece, piece), :]

    def far_part(hop, e):
        return w_at(slot_of(hop, 0, 0), e) if e < pieces else w_at(slot_of(hop, 1, 0), last)

    def wfar_copy(hop, e):
        ref = far_part(0, e)
        return remote(ref, ref, wfar_send.at[hop, e], wfar_recv.at[hop, e], "ctx", far[hop])

    def wpass_copy(e):
        ref = far_part(2, e)
        return remote(ref, ref, wpass_send.at[e], wfar_recv.at[3, e], "ctx", far[1])

    def wside_copy(hop, n):
        ref = w_at(far[hop], n)
        return remote(ref, ref, wside_send.at[hop, n], wside_recv.at[hop, n], "ctx", side)

    def wpair_copy(hop, cross, n):
        ref = w_at(slot_of(hop, cross, 0), n)
        return remote(ref, ref, wpair_send.at[hop * 2 + cross, n], wpair_recv.at[hop * 2 + cross, n], "ctx", pair)

    def rows_copy(which, h):
        cols = pl.ds(pl.multiple_of(h * piece, piece), piece)
        return remote(
            rows_ref.at[pl.ds(which * half, half), cols],
            rows_ref.at[pl.ds(tokens + which * half, half), cols],
            rows_send.at[which, h],
            rows_recv.at[which, h],
            "groups",
            guest,
        )

    def back_copy(n, slot):
        cols = pl.ds(pl.multiple_of((slot * 2 + part) * share, share), share)
        return remote(back_ref.at[n], out_ref.at[:, cols], back_send.at[n], back_recv.at[n], "groups", guest)

    def far_start(copy, hop):
        if hop == 3:

            @pl.when(inside)
            def _():
                copy.start()

        else:
            copy.start()

    def pass_on(copy):
        @pl.when(inside)
        def _():
            copy.start()

    def far_arrived(item, hop):
        far_copy(item, hop).wait_recv()
        if hop == 2:
            pass_on(pass_copy(item))
        side_copy(item, hop).start()
        pair_copy(item, hop, 0).start()

    def side_arrived(item, hop):
        side_copy(item, hop).wait_recv()
        pair_copy(item, hop, 1).start()

    def pair_arrived(item, hop):
        for cross in range(2):
            pair_copy(item, hop, cross).wait_recv()

    def wfar_arrived(hop, e):
        wfar_copy(hop, e).wait_recv()
        if hop == 2:
            pass_on(wpass_copy(e))
        if e < last:
            wside_copy(hop, e).start()
        wpair_copy(hop, 1 if e == pieces else 0, min(e, last)).start()

    def wside_arrived(hop, n):
        wside_copy(hop, n).wait_recv()
        wpair_copy(hop, 1, n).start()

    own_weight = pltpu.make_async_copy(
        w_ref.at[:, pl.ds(pl.multiple_of(part * share, share), share)], w_all.at[me], own_sem
    )
    own_weight.start()
    queries = pltpu.make_async_copy(q_raw, q_in, q_sem)
    queries.start()
    def own_start(item):
        for hop in range(1, outers):
            far_start(far_copy(item, hop), hop)

    for item in range(2):
        side_copy(item, 0).start()
        own_start(item)
        pair_copy(item, 0, 0).start()
    pair_copy(2, 0, 0).start()
    kv_low[me] = kv_ref[:half, :]
    kv_high[me] = kv_ref[half:, :]
    firsts[me] = table_ref[...]

    def clear(at):
        max_ref[at] = jnp.full(max_ref.shape[1:], LOW_START, jnp.float32)
        sum_ref[at] = jnp.zeros(sum_ref.shape[1:], jnp.float32)
        acc_ref[at] = jnp.zeros(acc_ref.shape[1:], jnp.float32)

    for h in range(kv_heads):
        clear(h)
    queries.wait()
    for h in range(kv_heads):
        for which in range(2):
            mine = q_in[which * half : (which + 1) * half, h * group : (h + 1) * group, :]
            q_ref[h, which] = mine.reshape(width, head_size)
    own_weight.wait()

    def step(h, which, source, places, at, visible):
        keys = pl.ds(pl.multiple_of(h * head_size, head_size), head_size)
        values = pl.ds(pl.multiple_of((kv_heads + h) * head_size, head_size), head_size)
        key_part = jnp.concatenate([source[p, :, keys] for p in places], axis=0)
        value_part = jnp.concatenate([source[p, :, values] for p in places], axis=0)
        scores = lax.dot_general(
            key_part, q_ref[h, which], (((1,), (1,)), ((), ())), preferred_element_type=jnp.float32
        )
        old_max = max_ref[at]
        if visible is not None:
            scores = jnp.where(visible, scores, LOW_START)
        new_max = jnp.maximum(old_max, jnp.max(scores, axis=0, keepdims=True))
        factor = jnp.exp2((old_max - new_max) * to_exp2)
        exp_scores = jnp.exp2((scores - new_max) * to_exp2)
        max_ref[at] = new_max
        sum_ref[at] = sum_ref[at] * factor + jnp.sum(exp_scores, axis=0, keepdims=True)
        weighted = lax.dot_general(
            value_part,
            exp_scores.astype(jnp.bfloat16),
            (((0,), (0,)), ((), ())),
            preferred_element_type=jnp.float32,
        )
        acc_ref[at] = acc_ref[at] * factor + weighted

    def run_hooks(number, hooks):
        for at, actions in hooks.items():

            @pl.when(number == at)
            def _():
                for action in actions:
                    action()

    def low_blocks(parts, hooks):
        places = [slot_of(hop, cross, swap) for hop, cross in parts for swap in range(2)]
        for hop, cross in parts:
            for item in range(2):
                pair_copy(item, hop, cross).wait_recv()

        @pl.loop(0, kv_heads)
        def _(h):
            run_hooks(h, hooks)
            step(h, 1, kv_low, places, h, None)

    def low_side(hop):
        for item in range(2):
            side_arrived(item, hop)

    def low_far(hop):
        for item in range(2):
            far_arrived(item, hop)

    def weight_round(e):
        for hop in (2, 1, 3):
            far_start(wfar_copy(hop, e), hop)

    def weight_own(n):
        wside_copy(0, n).start()
        wpair_copy(0, 0, n).start()

    def do(action, *args):
        return functools.partial(action, *args)

    low_side(0)
    low_blocks([(0, 0), (0, 1)], {3: [do(low_far, 1)]})
    low_far(2)
    own_start(2)
    low_blocks([(1, 0), (2, 0)], {2: [side_copy(2, 0).start]})
    low_side(1)
    low_far(3)
    low_blocks([(1, 1), (3, 0)], {1: [do(low_side, 2)], 3: [do(far_arrived, 2, 1)]})
    far_arrived(2, 2)
    weight_round(0)
    low_side(3)

    def find_places():
        lanes = lax.broadcasted_iota(jnp.int32, (1, half), 1)
        numbers = jnp.zeros((1, half), jnp.int32)
        for d in range(devices):
            for i in range(2):
                numbers = numbers + jnp.where(firsts[d, i : i + 1, :] // half == lanes, d, 0)
        place_vec[...] = jnp.broadcast_to(jnp.minimum(numbers, devices - 1), place_vec.shape)

    low_blocks([(2, 1), (3, 1)], {0: [do(side_arrived, 2, 0)], 1: [do(weight_own, last), find_places], 2: [do(weight_round, 1)]})
    to_scalars = pltpu.make_async_copy(place_vec, place_ref, place_sem)
    to_scalars.start()
    to_scalars.wait()

    first = order_ref[0] // half
    key_rows = lax.broadcasted_iota(jnp.int32, (span, width), 0)
    query_cols = lax.broadcasted_iota(jnp.int32, (span, width), 1) // group

    def finish(which, hooks):
        block = blocks - 1 - first if which else first

        @pl.loop(0, kv_heads)
        def _(h):
            at = h if which else kv_heads
            if not which:
                clear(at)

            @pl.loop(0, groups)
            def _(t):
                run_hooks(h * groups + t, hooks)

                @pl.when(jnp.logical_and(t == 1, h > 0))
                def _():
                    rows_copy(which, h - 1).start()

                number = groups + t if which else t
                places = [place_ref[0, number * BLOCKS_PER_STEP + i] for i in range(BLOCKS_PER_STEP)]
                visible = number * span + key_rows <= block * half + query_cols
                step(h, which, kv_high if which else kv_low, places, at, visible)

            for g in range(group):
                cols = pl.ds(g * half, half)
                attended = acc_ref[at, :, cols] / sum_ref[at, :, cols]
                turn_ref[cols, :] = attended.T
            for g in range(group):
                target = pl.ds(pl.multiple_of(h * piece + g * head_size, head_size), head_size)
                mine = turn_ref[pl.ds(g, half, stride=group), :]
                rows_ref[pl.ds(which * half, half), target] = mine.astype(jnp.bfloat16)

    finish(
        0,
        {
            0: [do(weight_own, 0)],
            1: [do(side_arrived, 2, 1)],
            3: [do(far_arrived, 2, 3)],
            5: [do(side_arrived, 2, 2), do(weight_own, 1)],
            8: [do(wfar_arrived, 1, 0), do(weight_own, 2)],
            9: [do(weight_round, 2)],
            10: [do(wfar_arrived, 2, 0)],
            12: [do(side_arrived, 2, 3)],
            14: [do(wfar_arrived, 1, 1)],
        },
    )
    for hop in range(outers):
        pair_arrived(2, hop)
    rows_copy(0, kv_heads - 1).start()
    finish(
        1,
        {
            0: [do(wside_arrived, 0, last)],
            1: [do(wfar_arrived, 2, 1)],
            2: [do(wfar_arrived, 3, 0)],
            3: [do(weight_round, last)],
            5: [do(wside_arrived, 0, 0)],
            8: [do(wfar_arrived, 1, 2)],
            9: [do(wside_arrived, 0, 1)],
            10: [do(weight_round, pieces)],
            11: [do(wfar_arrived, 2, 2)],
            12: [do(wfar_arrived, 3, 1)],
            14: [do(wside_arrived, 0, 2), do(wside_arrived, 1, 0)],
        },
    )
    wside_arrived(2, 0)
    rows_copy(1, kv_heads - 1).start()

    def project(hop, cross, low, high, begin=False, end=False):
        n = hop * 2 + cross
        base = slot_of(hop, cross, 0) - inner
        for m in range(low, high):
            wpair_copy(hop, cross, m).wait_recv()
        deep = pl.ds(low * piece, (high - low) * piece)
        weight = jnp.concatenate([w_all[base, deep, :], w_all[base + 1, deep, :]], axis=1)
        product = lax.dot_general(
            rows_ref[:, deep], weight, (((1,), (0,)), ((), ())), preferred_element_type=jnp.float32
        )
        if not begin:
            product = product + part_ref[n]
        if not end:
            part_ref[n] = product
            return
        product = product.astype(jnp.bfloat16)
        for i in range(2):
            back_ref[n * 2 + i] = product[tokens:, i * share : (i + 1) * share]
        for i in range(2):
            cols = pl.ds(pl.multiple_of(((base + i) * 2 + part) * share, share), share)
            out_ref[:, cols] = product[:tokens, i * share : (i + 1) * share]
        for i in range(2):
            back_copy(n * 2 + i, base + i).start()

    for which in range(2):
        for h in range(kv_heads):
            rows_copy(which, h).wait_recv()
    project(0, 0, 0, pieces, True, True)
    wside_arrived(3, 0)
    wside_arrived(1, 1)
    project(0, 1, 0, pieces, True, True)
    wfar_arrived(3, 2)
    wfar_arrived(1, last)
    wfar_arrived(2, last)
    project(1, 0, 0, last, True)
    project(2, 0, 0, last, True)
    wside_arrived(2, 1)
    wfar_arrived(1, pieces)

    for which in range(2):
        for h in range(kv_heads):
            rows_copy(which, h).wait_send()
    for hop in range(outers):
        for item in range(3):
            if 0 < hop < 3:
                far_copy(item, hop).wait_send()
            side_copy(item, hop).wait_send()
            for cross in range(2):
                pair_copy(item, hop, cross).wait_send()

    wfar_arrived(2, pieces)
    project(1, 0, last, pieces, False, True)
    project(2, 0, last, pieces, False, True)
    wside_arrived(1, 2)
    project(1, 1, 0, pieces, True, True)
    for hop in range(1, 3):
        for e in range(last):
            wfar_copy(hop, e).wait_send()
    for n in range(pieces):
        wside_copy(0, n).wait_send()
        for cross in range(2):
            wpair_copy(0, cross, n).wait_send()

    @pl.when(inside)
    def _():
        for item in range(3):
            far_copy(item, 3).wait_send()
            pass_copy(item).wait_send()
        for e in range(last):
            wfar_copy(3, e).wait_send()
            wpass_copy(e).wait_send()

    wside_arrived(3, 1)
    project(3, 0, 0, last, True)
    wfar_arrived(3, last)
    wside_arrived(2, 2)
    project(2, 1, 0, pieces, True, True)
    project(3, 1, 0, 2, True)
    wfar_arrived(3, pieces)
    wside_arrived(3, 2)
    project(3, 0, last, pieces, False, True)
    project(3, 1, 2, pieces, False, True)

    for hop in range(1, outers):
        for n in range(pieces):
            if n < last:
                wside_copy(hop, n).wait_send()
            for cross in range(2):
                wpair_copy(hop, cross, n).wait_send()
        for e in range(last, pieces + 1):
            if hop < 3:
                wfar_copy(hop, e).wait_send()

    @pl.when(inside)
    def _():
        for e in range(last, pieces + 1):
            wfar_copy(3, e).wait_send()
            wpass_copy(e).wait_send()

    for n in range(2 * 2 * outers):
        back_copy(n, 0).wait_send()
    for n in range(2 * 2 * outers):
        back_copy(n, 0).wait_recv()


def layer(query_states, packed, positions, out_weight, kv_heads):
    devices = lax.axis_size("ctx")
    outers = devices // 4
    tokens, query_heads, head_size = query_states.shape
    half = tokens // 2
    group = query_heads // kv_heads
    width = group * half
    depth, columns = out_weight.shape
    share = columns // 2
    slots = kv_heads + 1
    pieces = kv_heads
    dma = pltpu.SemaphoreType.DMA
    flops = 4 * query_states.size * half * (2 * devices + 1) // 2 + 4 * tokens * depth * columns * devices // 2
    return pl.pallas_call(
        functools.partial(layer_kernel, (devices, half, kv_heads, group, head_size, share)),
        out_shape=jax.ShapeDtypeStruct((tokens, columns * devices), jnp.bfloat16),
        in_specs=[
            pl.BlockSpec(memory_space=pltpu.SMEM),
            pl.BlockSpec(memory_space=pltpu.VMEM),
            pl.BlockSpec(memory_space=pltpu.VMEM),
            pl.BlockSpec(memory_space=pl.ANY),
            pl.BlockSpec(memory_space=pl.ANY),
        ],
        out_specs=pl.BlockSpec(memory_space=pltpu.VMEM),
        scratch_shapes=[
            pltpu.VMEM((devices, half, packed.shape[1]), packed.dtype),
            pltpu.VMEM((devices, half, packed.shape[1]), packed.dtype),
            pltpu.VMEM((devices, 2, half), jnp.int32),
            pltpu.VMEM((8, half), jnp.int32),
            pltpu.SMEM((8, half), jnp.int32),
            pltpu.VMEM((devices, depth, share), out_weight.dtype),
            pltpu.VMEM((slots, head_size, width), jnp.float32),
            pltpu.VMEM((slots, 1, width), jnp.float32),
            pltpu.VMEM((slots, 1, width), jnp.float32),
            pltpu.VMEM((2 * tokens, depth), jnp.bfloat16),
            pltpu.VMEM((devices, tokens, share), jnp.bfloat16),
            pltpu.VMEM((devices // 2, 2 * tokens, 2 * share), jnp.float32),
            pltpu.VMEM(query_states.shape, query_states.dtype),
            pltpu.VMEM((kv_heads, 2, width, head_size), query_states.dtype),
            pltpu.VMEM((width, head_size), jnp.float32),
            dma((3, outers)),
            dma((3, outers)),
            dma((3, outers)),
            dma((3, outers)),
            dma((3, 2 * outers)),
            dma((3, 2 * outers)),
            dma((outers, pieces + 1)),
            dma((outers, pieces + 1)),
            dma((outers, pieces)),
            dma((outers, pieces)),
            dma((2 * outers, pieces)),
            dma((2 * outers, pieces)),
            dma((2, kv_heads)),
            dma((2, kv_heads)),
            dma((devices,)),
            dma((devices,)),
            dma((3,)),
            dma((pieces + 1,)),
            dma,
            dma,
            dma,
        ],
        compiler_params=pltpu.CompilerParams(
            collective_id=0, has_side_effects=True, vmem_limit_bytes=VMEM
        ),
        cost_estimate=pl.CostEstimate(flops=flops, bytes_accessed=2 * out_weight.size, transcendentals=0),
        name="layer",
    )(positions, positions.reshape(2, half), packed, query_states, out_weight)


def local(query_states, key_states, value_rows, positions, out_weight):
    tokens, query_heads, head_size = query_states.shape
    kv_heads = key_states.shape[1]
    group = query_heads // kv_heads
    half = tokens // 2
    devices = lax.axis_size("ctx")
    blocks = 2 * devices
    parts = lax.axis_size("groups")
    me_part = lax.axis_index("groups")
    share = out_weight.shape[1] // parts
    if parts == 2 and lax.axis_size("tp") == 1 and devices == 4 * BLOCKS_PER_STEP and share % 128 == 0:
        packed = jnp.concatenate(
            [key_states.reshape(tokens, kv_heads * head_size), value_rows.reshape(tokens, kv_heads * head_size)], axis=1
        )
        return layer(query_states, packed, positions, out_weight, kv_heads)
    query_parts = query_states.reshape(2, half, kv_heads, group, head_size).transpose(2, 0, 3, 1, 4)
    query_parts = query_parts.reshape(kv_heads, 2, group * half, head_size)
    weight_share = lax.dynamic_slice_in_dim(out_weight, me_part * share, share, 1)
    weight = lax.all_gather(weight_share, "ctx", axis=1, tiled=True)
    packed = jnp.concatenate(
        [key_states.reshape(tokens, kv_heads * head_size), value_rows.reshape(tokens, kv_heads * head_size)], axis=1
    )
    first = positions[0] // half
    tail = jnp.broadcast_to(first.astype(packed.dtype), (TAIL, packed.shape[1]))
    gathered = spread(jnp.concatenate([packed, tail], axis=0))
    firsts = gathered[:, tokens, 0].astype(jnp.int32)
    gathered = gathered.reshape(devices * (tokens + TAIL), packed.shape[1])
    wanted = jnp.arange(blocks, dtype=jnp.int32)[:, None]
    stored = jnp.stack([firsts, blocks - 1 - firsts], axis=1).reshape(1, blocks)
    kept = jnp.arange(blocks, dtype=jnp.int32)[None, :]
    starts = kept // 2 * (tokens + TAIL) + kept % 2 * half
    place = jnp.sum(jnp.where(stored == wanted, starts, 0), axis=1)
    place = place.astype(jnp.int32)
    own = jnp.stack([first, blocks - 1 - first]).astype(jnp.int32)
    pieces = min(2, kv_heads)
    span = kv_heads // pieces
    attended = [
        attend(query_parts[i * span : (i + 1) * span], gathered, place, own, i * span, kv_heads, half) for i in range(pieces)
    ]

    def project(rows):
        product = lax.dot_general(
            jnp.concatenate(rows, axis=0), weight, (((0,), (0,)), ((), ())), preferred_element_type=jnp.float32
        )
        return product.astype(jnp.bfloat16)

    guests = [[hand_on(piece, by) for piece in attended] for by in range(1, parts)]
    mine = project(attended)
    results = [mine] + [hand_on(project(rows), parts - 1 - i) for i, rows in enumerate(guests)]
    if share % 128 == 0:
        combined = weave(results, me_part, devices)
    else:
        shares = jnp.stack([r.reshape(tokens, devices, share) for r in results])
        order = (jnp.arange(parts) - me_part) % parts
        combined = jnp.moveaxis(jnp.take(shares, order, axis=0), 0, 2).reshape(tokens, devices * parts * share)
    return lax.psum_scatter(combined, "tp", scatter_dimension=1, tiled=True)


def solution(mesh):
    in_specs = (
        P(("groups", "ctx"), "tp", None),
        P(("groups", "ctx"), "tp", None),
        P(("groups", "ctx"), "tp", None),
        P(("groups", "ctx")),
        P("tp", "ctx"),
    )
    out_specs = P(("groups", "ctx"), "tp")
    return jax.shard_map(local, mesh=mesh, in_specs=in_specs, out_specs=out_specs, check_vma=False)
```

```python
import functools
import math

import jax
import jax.numpy as jnp
from jax import lax
from jax.experimental import pallas as pl
from jax.experimental.pallas import tpu as pltpu
from jax.sharding import PartitionSpec as P

LOW_START = -1e30
BLOCKS_PER_STEP = 4
CHUNK = 1024
TAIL = 16
VMEM = 50 * 1024 * 1024


def attend_kernel(half, group, place_ref, own_ref, q_ref, k_ref, v_ref, out_ref, acc_ref, max_ref, sum_ref):
    rows = group * half
    head_size = q_ref.shape[-1]
    span = BLOCKS_PER_STEP * half
    chunk = min(CHUNK, rows)
    to_exp2 = head_size ** (-0.5) * math.log2(math.e)

    def step(which, number, masked, query_block):
        keys, values = [], []
        for i in range(BLOCKS_PER_STEP):
            place = place_ref[number * BLOCKS_PER_STEP + i]
            keys.append(k_ref[pl.ds(pl.multiple_of(place, TAIL), half), :])
            values.append(v_ref[pl.ds(pl.multiple_of(place, TAIL), half), :])
        key_part = jnp.concatenate(keys, axis=0)
        value_part = jnp.concatenate(values, axis=0)
        if masked:
            key_place = number * span + lax.broadcasted_iota(jnp.int32, (span, chunk), 0)
            query_place = query_block * half + lax.broadcasted_iota(jnp.int32, (span, chunk), 1) % half
            visible = key_place <= query_place
        for c in range(rows // chunk):
            cols = pl.ds(c * chunk, chunk)
            scores = lax.dot_general(
                key_part,
                q_ref[0, which, cols, :],
                (((1,), (1,)), ((), ())),
                preferred_element_type=jnp.float32,
            )
            if masked:
                scores = jnp.where(visible, scores, LOW_START)
            old_max = max_ref[:, cols]
            new_max = jnp.maximum(old_max, jnp.max(scores, axis=0, keepdims=True))
            factor = jnp.exp2((old_max - new_max) * to_exp2)
            exp_scores = jnp.exp2((scores - new_max) * to_exp2)
            max_ref[:, cols] = new_max
            sum_ref[:, cols] = sum_ref[:, cols] * factor + jnp.sum(exp_scores, axis=0, keepdims=True)
            weighted = lax.dot_general(
                value_part,
                exp_scores.astype(jnp.bfloat16),
                (((0,), (0,)), ((), ())),
                preferred_element_type=jnp.float32,
            )
            acc_ref[:, cols] = acc_ref[:, cols] * factor + weighted

    for which in range(2):
        query_block = own_ref[which]
        steps = query_block // BLOCKS_PER_STEP
        max_ref[...] = jnp.full_like(max_ref, LOW_START)
        sum_ref[...] = jnp.zeros_like(sum_ref)
        acc_ref[...] = jnp.zeros_like(acc_ref)

        @pl.loop(0, steps)
        def _(number):
            step(which, number, False, query_block)

        step(which, steps, True, query_block)
        for g in range(group):
            cols = pl.ds(g * half, half)
            attended = acc_ref[:, cols] / sum_ref[:, cols]
            out_ref[pl.ds(g * head_size, head_size), pl.ds(which * half, half)] = attended.astype(jnp.bfloat16)


def attend(query_parts, gathered, place, own, first_head, all_heads, half):
    kv_heads, _, rows, head_size = query_parts.shape
    keys_total = gathered.shape[0]
    blocks = place.shape[0]
    group = rows // half
    flops = 4 * kv_heads * rows * head_size * half * (blocks + 1)
    return pl.pallas_call(
        functools.partial(attend_kernel, half, group),
        out_shape=jax.ShapeDtypeStruct((kv_heads * group * head_size, 2 * half), jnp.bfloat16),
        grid_spec=pltpu.PrefetchScalarGridSpec(
            num_scalar_prefetch=2,
            grid=(kv_heads,),
            in_specs=[
                pl.BlockSpec((1, 2, rows, head_size), lambda h, *_: (h, 0, 0, 0)),
                pl.BlockSpec((keys_total, head_size), lambda h, *_: (0, h + first_head)),
                pl.BlockSpec((keys_total, head_size), lambda h, *_: (0, h + first_head + all_heads)),
            ],
            out_specs=pl.BlockSpec((group * head_size, 2 * half), lambda h, *_: (h, 0)),
            scratch_shapes=[
                pltpu.VMEM((head_size, rows), jnp.float32),
                pltpu.VMEM((1, rows), jnp.float32),
                pltpu.VMEM((1, rows), jnp.float32),
            ],
        ),
        compiler_params=pltpu.CompilerParams(
            dimension_semantics=("arbitrary",), vmem_limit_bytes=20 * 1024 * 1024
        ),
        cost_estimate=pl.CostEstimate(
            flops=flops, bytes_accessed=2 * gathered.size, transcendentals=flops // (4 * head_size)
        ),
        name="attend",
    )(place, own, query_parts, gathered, gathered)


def spread_kernel(devices, own_ref, out_ref, far_send, far_recv, side_send, side_recv, pair_send, pair_recv, own_sem):
    me = lax.axis_index("ctx")
    outers = devices // 4
    outer, middle, inner = me // 4, (me // 2) % 2, me % 2

    def at(o, m, i):
        return (o * 2 + m) * 2 + i

    side = at(outer, 1 - middle, inner)
    pair = at(outer, middle, 1 - inner)
    far = [at((outer + k) % outers, middle, inner) for k in range(1, outers)]
    barrier = pltpu.get_barrier_semaphore()
    for other in far + [side, pair]:
        pl.semaphore_signal(barrier, inc=1, device_id={"ctx": other}, device_id_type=pl.DeviceIdType.MESH)
    pl.semaphore_wait(barrier, outers + 1)

    def send(source, slot, sends, recvs, number, target):
        return pltpu.make_async_remote_copy(
            src_ref=source,
            dst_ref=out_ref.at[slot],
            send_sem=sends.at[number],
            recv_sem=recvs.at[number],
            device_id={"ctx": target},
            device_id_type=pl.DeviceIdType.MESH,
        )

    own = pltpu.make_async_copy(own_ref, out_ref.at[me], own_sem)
    far_copies = [send(own_ref, me, far_send, far_recv, k, far[k]) for k in range(outers - 1)]
    for copy in far_copies:
        copy.start()
    side_copies = [send(own_ref, me, side_send, side_recv, 0, side)]
    pair_copies = [send(own_ref, me, pair_send, pair_recv, 0, pair)]
    side_copies[0].start()
    pair_copies[0].start()
    own.start()
    for k in range(outers - 1):
        far_copies[k].wait_recv()
        slot = at((outer + outers - 1 - k) % outers, middle, inner)
        side_copies.append(send(out_ref.at[slot], slot, side_send, side_recv, k + 1, side))
        pair_copies.append(send(out_ref.at[slot], slot, pair_send, pair_recv, k + 1, pair))
        side_copies[-1].start()
        pair_copies[-1].start()
    for k in range(outers):
        side_copies[k].wait_recv()
        slot = at((outer + outers - k) % outers, 1 - middle, inner)
        pair_copies.append(send(out_ref.at[slot], slot, pair_send, pair_recv, outers + k, pair))
        pair_copies[-1].start()
    for copy in pair_copies:
        copy.wait_recv()
    for copy in far_copies + side_copies + pair_copies:
        copy.wait_send()
    own.wait()


def spread(packed):
    devices = lax.axis_size("ctx")
    outers = devices // 4
    rows, columns = packed.shape
    gathered = pl.pallas_call(
        functools.partial(spread_kernel, devices),
        out_shape=jax.ShapeDtypeStruct((devices, rows, columns), packed.dtype),
        in_specs=[pl.BlockSpec(memory_space=pltpu.VMEM)],
        out_specs=pl.BlockSpec(memory_space=pltpu.VMEM),
        scratch_shapes=[
            pltpu.SemaphoreType.DMA((outers - 1,)),
            pltpu.SemaphoreType.DMA((outers - 1,)),
            pltpu.SemaphoreType.DMA((outers,)),
            pltpu.SemaphoreType.DMA((outers,)),
            pltpu.SemaphoreType.DMA((2 * outers,)),
            pltpu.SemaphoreType.DMA((2 * outers,)),
            pltpu.SemaphoreType.DMA,
        ],
        compiler_params=pltpu.CompilerParams(
            collective_id=0, has_side_effects=True, vmem_limit_bytes=24 * 1024 * 1024
        ),
        cost_estimate=pl.CostEstimate(flops=0, bytes_accessed=20 * packed.size * devices, transcendentals=0),
        name="spread",
    )(packed)
    return gathered


def hand_on(value, by):
    parts = lax.axis_size("groups")
    return lax.ppermute(value, "groups", [(i, (i + by) % parts) for i in range(parts)])


def weave_kernel(share, me_ref, *refs):
    *shares, out_ref = refs
    parts = len(shares)
    for p in range(parts):
        by = lax.rem(p - me_ref[0] + parts, parts)
        chosen = shares[0][...]
        for k in range(1, parts):
            chosen = jnp.where(by == k, shares[k][...], chosen)
        for i in range(chosen.shape[1] // share):
            out_ref[:, (i * parts + p) * share : (i * parts + p + 1) * share] = chosen[:, i * share : (i + 1) * share]


def weave(results, me_part, devices):
    parts = len(results)
    tokens, columns = results[0].shape
    share = columns // devices
    return pl.pallas_call(
        functools.partial(weave_kernel, share),
        out_shape=jax.ShapeDtypeStruct((tokens, parts * columns), results[0].dtype),
        grid_spec=pltpu.PrefetchScalarGridSpec(
            num_scalar_prefetch=1,
            grid=(devices // 4,),
            in_specs=[pl.BlockSpec((tokens, 4 * share), lambda i, *_: (0, i))] * parts,
            out_specs=pl.BlockSpec((tokens, 4 * parts * share), lambda i, *_: (0, i)),
        ),
        name="weave",
    )(me_part.astype(jnp.int32).reshape(1), *results)


def layer_kernel(sizes, order_ref, table_ref, kv_ref, q_raw, w_ref, out_ref, *scratch):
    devices, half, kv_heads, group, head_size, share = sizes
    (kv_low, kv_high, firsts, place_vec, place_ref, w_all, acc_ref, max_ref, sum_ref, rows_ref, back_ref, part_ref, q_in, q_ref, turn_ref, *sems) = scratch
    (far_send, far_recv, side_recv, pair_send, pair_recv, wfar_send, wfar_recv, wside_send, wside_recv) = sems[:9]
    (wpair_send, wpair_recv, rows_send, rows_recv, back_send, back_recv, own_sem, place_sem, q_sem) = sems[9:]
    outers = devices // 4
    blocks = 2 * devices
    tokens = 2 * half
    width = group * half
    depth = kv_heads * group * head_size
    pieces = kv_heads
    piece = depth // pieces
    span = BLOCKS_PER_STEP * half
    groups = devices // BLOCKS_PER_STEP
    to_exp2 = head_size ** (-0.5) * math.log2(math.e)

    part = lax.axis_index("groups")
    me = lax.axis_index("ctx")
    outer, middle, inner = me // 4, (me // 2) % 2, me % 2

    def flip(number, by):
        result, unit = 0, 1
        while unit < outers:
            result = result + (number // unit + by // unit) % 2 * unit
            unit *= 2
        return result

    def slot_of(hop, cross, swap):
        return (flip(outer, hop) * 2 + (middle + cross) % 2) * 2 + (inner + swap) % 2

    far = [slot_of(k, 0, 0) for k in range(outers)]
    side = slot_of(0, 1, 0)
    pair = slot_of(0, 0, 1)
    inside = jnp.logical_and(outer > 0, outer < outers - 1)
    last = pieces - 1
    guest = lax.rem(part + 1, 2)

    barrier = pltpu.get_barrier_semaphore()
    for other in far[1:] + [side, pair]:
        pl.semaphore_signal(barrier, inc=1, device_id={"ctx": other}, device_id_type=pl.DeviceIdType.MESH)
    pl.semaphore_signal(barrier, inc=1, device_id={"groups": guest}, device_id_type=pl.DeviceIdType.MESH)
    pl.semaphore_wait(barrier, outers + 2)

    def remote(source, target, send, recv, axis, index):
        return pltpu.make_async_remote_copy(
            src_ref=source,
            dst_ref=target,
            send_sem=send,
            recv_sem=recv,
            device_id={axis: index},
            device_id_type=pl.DeviceIdType.MESH,
        )

    def own_item(item):
        return table_ref if item == 0 else kv_ref.at[pl.ds((item - 1) * half, half), :]

    def item_at(item, slot):
        if item == 0:
            return firsts.at[slot]
        return (kv_low if item == 1 else kv_high).at[slot]

    def source_of(item, hop, cross):
        return own_item(item) if hop == 0 and cross == 0 else item_at(item, slot_of(hop, cross, 0))

    def far_copy(item, hop):
        return remote(own_item(item), item_at(item, me), far_send.at[item, hop // 3], far_recv.at[item, hop], "ctx", far[hop])

    def pass_copy(item):
        ref = item_at(item, far[2])
        return remote(ref, ref, far_send.at[item, 1], far_recv.at[item, 3], "ctx", far[1])

    def side_copy(item, hop):
        return remote(
            source_of(item, hop, 0), item_at(item, far[hop]), pair_send.at[item], side_recv.at[item, hop], "ctx", side
        )

    def pair_copy(item, hop, cross):
        n = hop * 2 + cross
        return remote(
            source_of(item, hop, cross),
            item_at(item, slot_of(hop, cross, 0)),
            pair_send.at[item],
            pair_recv.at[n if item == 1 else 2 * outers + item // 2],
            "ctx",
            pair,
        )

    def w_at(slot, n):
        return w_all.at[slot, pl.ds(n * piece, piece), :]

    def far_part(hop, e):
        return w_at(slot_of(hop, 0, 0), e) if e < pieces else w_at(slot_of(hop, 1, 0), last)

    def wfar_copy(hop, e):
        ref = far_part(0, e)
        return remote(ref, ref, wfar_send.at[hop], wfar_recv.at[hop, e], "ctx", far[hop])

    def wpass_copy(e):
        ref = far_part(2, e)
        return remote(ref, ref, wfar_send.at[0], wfar_recv.at[3, e], "ctx", far[1])

    def wside_copy(hop, n):
        ref = w_at(far[hop], n)
        return remote(ref, ref, wside_send.at[min(hop, 1)], wside_recv.at[hop, n], "ctx", side)

    def wpair_copy(hop, cross, n):
        ref = w_at(slot_of(hop, cross, 0), n)
        return remote(ref, ref, wpair_send.at[hop], wpair_recv.at[hop * 2 + cross, n], "ctx", pair)

    def rows_copy(which, h):
        cols = pl.ds(pl.multiple_of(h * piece, piece), piece)
        return remote(
            rows_ref.at[pl.ds(which * half, half), cols],
            rows_ref.at[pl.ds(tokens + which * half, half), cols],
            rows_send,
            rows_recv,
            "groups",
            guest,
        )

    def back_copy(n, slot):
        cols = pl.ds(pl.multiple_of((slot * 2 + part) * share, share), share)
        return remote(back_ref.at[n], out_ref.at[:, cols], back_send, back_recv, "groups", guest)

    def all_sent(ref, sem):
        remote(ref, ref, sem, sem, "ctx", pair).wait_send()

    def all_landed(ref, sem):
        remote(ref, ref, sem, sem, "ctx", pair).wait_recv()

    def far_start(copy, hop):
        if hop == 3:

            @pl.when(inside)
            def _():
                copy.start()

        else:
            copy.start()

    def pass_on(copy):
        @pl.when(inside)
        def _():
            copy.start()

    def far_arrived(item, hop):
        far_copy(item, hop).wait_recv()
        if hop == 2:
            pass_on(pass_copy(item))
        side_copy(item, hop).start()
        pair_copy(item, hop, 0).start()

    def side_arrived(item, hop):
        side_copy(item, hop).wait_recv()
        pair_copy(item, hop, 1).start()

    def wfar_arrived(hop, e):
        wfar_copy(hop, e).wait_recv()
        if hop == 2:
            pass_on(wpass_copy(e))
        if e < last:
            wside_copy(hop, e).start()
        wpair_copy(hop, 1 if e == pieces else 0, min(e, last)).start()

    def wside_arrived(hop, n):
        wside_copy(hop, n).wait_recv()
        wpair_copy(hop, 1, n).start()

    own_weight = pltpu.make_async_copy(
        w_ref.at[:, pl.ds(pl.multiple_of(part * share, share), share)], w_all.at[me], own_sem
    )
    own_weight.start()
    queries = pltpu.make_async_copy(q_raw, q_in, q_sem)
    queries.start()
    def own_start(item):
        for hop in range(1, outers):
            far_start(far_copy(item, hop), hop)

    for item in range(2):
        side_copy(item, 0).start()
        own_start(item)
        pair_copy(item, 0, 0).start()
    pair_copy(2, 0, 0).start()
    kv_low[me] = kv_ref[:half, :]
    kv_high[me] = kv_ref[half:, :]
    firsts[me] = table_ref[...]

    def clear(at):
        max_ref[at] = jnp.full(max_ref.shape[1:], LOW_START, jnp.float32)
        sum_ref[at] = jnp.zeros(sum_ref.shape[1:], jnp.float32)
        acc_ref[at] = jnp.zeros(acc_ref.shape[1:], jnp.float32)

    for h in range(kv_heads):
        clear(h)
    queries.wait()
    for h in range(kv_heads):
        for which in range(2):
            mine = q_in[which * half : (which + 1) * half, h * group : (h + 1) * group, :]
            q_ref[h, which] = mine.reshape(width, head_size)
    own_weight.wait()

    def step(h, which, source, places, at, visible):
        keys = pl.ds(pl.multiple_of(h * head_size, head_size), head_size)
        values = pl.ds(pl.multiple_of((kv_heads + h) * head_size, head_size), head_size)
        key_part = jnp.concatenate([source[p, :, keys] for p in places], axis=0)
        value_part = jnp.concatenate([source[p, :, values] for p in places], axis=0)
        scores = lax.dot_general(
            key_part, q_ref[h, which], (((1,), (1,)), ((), ())), preferred_element_type=jnp.float32
        )
        old_max = max_ref[at]
        if visible is not None:
            scores = jnp.where(visible, scores, LOW_START)
        new_max = jnp.maximum(old_max, jnp.max(scores, axis=0, keepdims=True))
        factor = jnp.exp2((old_max - new_max) * to_exp2)
        exp_scores = jnp.exp2((scores - new_max) * to_exp2)
        max_ref[at] = new_max
        sum_ref[at] = sum_ref[at] * factor + jnp.sum(exp_scores, axis=0, keepdims=True)
        weighted = lax.dot_general(
            value_part,
            exp_scores.astype(jnp.bfloat16),
            (((0,), (0,)), ((), ())),
            preferred_element_type=jnp.float32,
        )
        acc_ref[at] = acc_ref[at] * factor + weighted

    def run_hooks(number, hooks):
        for at, actions in hooks.items():

            @pl.when(number == at)
            def _():
                for action in actions:
                    action()

    def low_blocks(parts, hooks):
        places = [slot_of(hop, cross, swap) for hop, cross in parts for swap in range(2)]
        for hop, cross in parts:
            pair_copy(1, hop, cross).wait_recv()

        @pl.loop(0, kv_heads)
        def _(h):
            run_hooks(h, hooks)
            step(h, 1, kv_low, places, h, None)

    def low_side(hop):
        for item in range(2):
            side_arrived(item, hop)

    def low_far(hop):
        for item in range(2):
            far_arrived(item, hop)

    def weight_round(e):
        for hop in (2, 1, 3):
            far_start(wfar_copy(hop, e), hop)

    def weight_own(n):
        wside_copy(0, n).start()
        wpair_copy(0, 0, n).start()

    def do(action, *args):
        return functools.partial(action, *args)

    low_side(0)
    side_copy(2, 0).start()
    low_blocks([(0, 0), (0, 1)], {2: [do(low_far, 1)]})
    low_far(2)
    own_start(2)
    low_blocks([(1, 0), (2, 0)], {})
    low_side(1)
    low_far(3)
    low_blocks([(1, 1), (3, 0)], {1: [do(low_side, 2)], 3: [do(far_arrived, 2, 1)]})
    far_arrived(2, 2)
    weight_round(0)
    low_side(3)

    def find_places():
        all_landed(firsts.at[pl.ds(0, 2 * outers)], pair_recv.at[2 * outers])
        lanes = lax.broadcasted_iota(jnp.int32, (1, half), 1)
        numbers = jnp.zeros((1, half), jnp.int32)
        for d in range(devices):
            for i in range(2):
                numbers = numbers + jnp.where(firsts[d, i : i + 1, :] // half == lanes, d, 0)
        place_vec[...] = jnp.broadcast_to(jnp.minimum(numbers, devices - 1), place_vec.shape)

    low_blocks([(2, 1), (3, 1)], {0: [do(side_arrived, 2, 0)], 1: [do(weight_own, last), find_places], 2: [do(weight_round, 1)]})
    to_scalars = pltpu.make_async_copy(place_vec, place_ref, place_sem)
    to_scalars.start()
    to_scalars.wait()

    first = order_ref[0] // half
    key_rows = lax.broadcasted_iota(jnp.int32, (span, width), 0)
    query_cols = lax.broadcasted_iota(jnp.int32, (span, width), 1) // group

    def finish(which, hooks):
        block = blocks - 1 - first if which else first

        @pl.loop(0, kv_heads)
        def _(h):
            at = h if which else kv_heads
            if not which:
                clear(at)

            @pl.loop(0, groups)
            def _(t):
                run_hooks(h * groups + t, hooks)

                @pl.when(jnp.logical_and(t == 1, h > 0))
                def _():
                    rows_copy(which, h - 1).start()

                number = groups + t if which else t
                places = [place_ref[0, number * BLOCKS_PER_STEP + i] for i in range(BLOCKS_PER_STEP)]
                visible = number * span + key_rows <= block * half + query_cols
                step(h, which, kv_high if which else kv_low, places, at, visible)

            for g in range(group):
                cols = pl.ds(g * half, half)
                attended = acc_ref[at, :, cols] / sum_ref[at, :, cols]
                turn_ref[cols, :] = attended.T
            for g in range(group):
                target = pl.ds(pl.multiple_of(h * piece + g * head_size, head_size), head_size)
                mine = turn_ref[pl.ds(g, half, stride=group), :]
                rows_ref[pl.ds(which * half, half), target] = mine.astype(jnp.bfloat16)

    finish(
        0,
        {
            0: [do(weight_own, 0)],
            1: [do(side_arrived, 2, 1)],
            3: [do(far_arrived, 2, 3)],
            5: [do(side_arrived, 2, 2), do(weight_own, 1)],
            8: [do(wfar_arrived, 1, 0), do(weight_own, 2)],
            9: [do(weight_round, 2)],
            10: [do(wfar_arrived, 2, 0)],
            12: [do(side_arrived, 2, 3)],
            14: [do(wfar_arrived, 1, 1)],
        },
    )
    all_landed(kv_high.at[pl.ds(0, 2 * outers)], pair_recv.at[2 * outers + 1])
    rows_copy(0, kv_heads - 1).start()
    finish(
        1,
        {
            0: [do(wside_arrived, 0, last)],
            1: [do(wfar_arrived, 2, 1)],
            2: [do(wfar_arrived, 3, 0)],
            3: [do(weight_round, last)],
            5: [do(wside_arrived, 0, 0)],
            8: [do(wfar_arrived, 1, 2)],
            9: [do(wside_arrived, 0, 1)],
            10: [do(weight_round, pieces)],
            11: [do(wfar_arrived, 2, 2)],
            12: [do(wfar_arrived, 3, 1)],
            14: [do(wside_arrived, 0, 2), do(wside_arrived, 1, 0)],
        },
    )
    wside_arrived(2, 0)
    rows_copy(1, kv_heads - 1).start()

    def project(hop, cross, low, high, begin=False, end=False):
        n = hop * 2 + cross
        base = slot_of(hop, cross, 0) - inner
        for m in range(low, high):
            wpair_copy(hop, cross, m).wait_recv()
        deep = pl.ds(low * piece, (high - low) * piece)
        weight = jnp.concatenate([w_all[base, deep, :], w_all[base + 1, deep, :]], axis=1)
        product = lax.dot_general(
            rows_ref[:, deep], weight, (((1,), (0,)), ((), ())), preferred_element_type=jnp.float32
        )
        if not begin:
            product = product + part_ref[n]
        if not end:
            part_ref[n] = product
            return
        product = product.astype(jnp.bfloat16)
        for i in range(2):
            back_ref[n * 2 + i] = product[tokens:, i * share : (i + 1) * share]
        for i in range(2):
            cols = pl.ds(pl.multiple_of(((base + i) * 2 + part) * share, share), share)
            out_ref[:, cols] = product[:tokens, i * share : (i + 1) * share]
        for i in range(2):
            back_copy(n * 2 + i, base + i).start()

    all_landed(rows_ref.at[pl.ds(tokens, tokens), :], rows_recv)
    project(0, 0, 0, pieces, True, True)
    wside_arrived(3, 0)
    wside_arrived(1, 1)
    wfar_arrived(3, 2)
    project(0, 1, 0, pieces, True, True)
    wfar_arrived(1, last)
    wfar_arrived(2, last)
    project(1, 0, 0, last, True)
    wside_arrived(2, 1)
    wfar_arrived(1, pieces)
    project(2, 0, 0, last, True)
    all_sent(rows_ref.at[pl.ds(0, tokens), :], rows_send)
    for item, ref in enumerate((firsts, kv_low, kv_high)):
        all_sent(ref.at[pl.ds(0, 2)], far_send.at[item, 0])
        all_sent(ref.at[pl.ds(0, 3 * outers)], pair_send.at[item])
    wfar_arrived(2, pieces)
    project(1, 0, last, pieces, False, True)
    project(2, 0, last, pieces, False, True)
    wside_arrived(1, 2)
    project(1, 1, 0, pieces, True, True)
    project(3, 0, 0, last, True)
    project(2, 1, 0, 2, True)
    wside_arrived(3, 1)
    wfar_arrived(3, last)
    project(3, 0, last, pieces, False, True)
    wside_arrived(2, 2)
    wfar_arrived(3, pieces)
    wside_arrived(3, 2)
    project(2, 1, 2, pieces, False, True)
    project(3, 1, 0, pieces, True, True)

    @pl.when(inside)
    def _():
        for item, ref in enumerate((firsts, kv_low, kv_high)):
            all_sent(ref.at[pl.ds(0, 2)], far_send.at[item, 1])
        for i in (0, 3):
            all_sent(w_all.at[pl.ds(0, pieces + 1), pl.ds(0, piece), :], wfar_send.at[i])

    for hop in range(1, 3):
        all_sent(w_all.at[pl.ds(0, pieces + 1), pl.ds(0, piece), :], wfar_send.at[hop])
    all_sent(w_all.at[0], wside_send.at[0])
    all_sent(w_all.at[pl.ds(0, outers - 1), pl.ds(0, last * piece), :], wside_send.at[1])
    for hop in range(outers):
        all_sent(w_all.at[pl.ds(0, 2)], wpair_send.at[hop])
    all_sent(back_ref, back_send)
    all_landed(back_ref, back_recv)


def layer(query_states, packed, positions, out_weight, kv_heads):
    devices = lax.axis_size("ctx")
    outers = devices // 4
    tokens, query_heads, head_size = query_states.shape
    half = tokens // 2
    group = query_heads // kv_heads
    width = group * half
    depth, columns = out_weight.shape
    share = columns // 2
    slots = kv_heads + 1
    pieces = kv_heads
    dma = pltpu.SemaphoreType.DMA
    flops = 4 * query_states.size * half * (2 * devices + 1) // 2 + 4 * tokens * depth * columns * devices // 2
    return pl.pallas_call(
        functools.partial(layer_kernel, (devices, half, kv_heads, group, head_size, share)),
        out_shape=jax.ShapeDtypeStruct((tokens, columns * devices), jnp.bfloat16),
        in_specs=[
            pl.BlockSpec(memory_space=pltpu.SMEM),
            pl.BlockSpec(memory_space=pltpu.VMEM),
            pl.BlockSpec(memory_space=pltpu.VMEM),
            pl.BlockSpec(memory_space=pl.ANY),
            pl.BlockSpec(memory_space=pl.ANY),
        ],
        out_specs=pl.BlockSpec(memory_space=pltpu.VMEM),
        scratch_shapes=[
            pltpu.VMEM((devices, half, packed.shape[1]), packed.dtype),
            pltpu.VMEM((devices, half, packed.shape[1]), packed.dtype),
            pltpu.VMEM((devices, 2, half), jnp.int32),
            pltpu.VMEM((8, half), jnp.int32),
            pltpu.SMEM((8, half), jnp.int32),
            pltpu.VMEM((devices, depth, share), out_weight.dtype),
            pltpu.VMEM((slots, head_size, width), jnp.float32),
            pltpu.VMEM((slots, 1, width), jnp.float32),
            pltpu.VMEM((slots, 1, width), jnp.float32),
            pltpu.VMEM((2 * tokens, depth), jnp.bfloat16),
            pltpu.VMEM((devices, tokens, share), jnp.bfloat16),
            pltpu.VMEM((devices // 2, 2 * tokens, 2 * share), jnp.float32),
            pltpu.VMEM(query_states.shape, query_states.dtype),
            pltpu.VMEM((kv_heads, 2, width, head_size), query_states.dtype),
            pltpu.VMEM((width, head_size), jnp.float32),
            dma((3, 2)),
            dma((3, outers)),
            dma((3, outers)),
            dma((3,)),
            dma((2 * outers + 2,)),
            dma((outers,)),
            dma((outers, pieces + 1)),
            dma((2,)),
            dma((outers, pieces)),
            dma((outers,)),
            dma((2 * outers, pieces)),
            dma,
            dma,
            dma,
            dma,
            dma,
            dma,
            dma,
        ],
        compiler_params=pltpu.CompilerParams(
            collective_id=0, has_side_effects=True, vmem_limit_bytes=VMEM
        ),
        cost_estimate=pl.CostEstimate(flops=flops, bytes_accessed=2 * out_weight.size, transcendentals=0),
        name="layer",
    )(positions, positions.reshape(2, half), packed, query_states, out_weight)


def local(query_states, key_states, value_rows, positions, out_weight):
    tokens, query_heads, head_size = query_states.shape
    kv_heads = key_states.shape[1]
    group = query_heads // kv_heads
    half = tokens // 2
    devices = lax.axis_size("ctx")
    blocks = 2 * devices
    parts = lax.axis_size("groups")
    me_part = lax.axis_index("groups")
    share = out_weight.shape[1] // parts
    if parts == 2 and lax.axis_size("tp") == 1 and devices == 4 * BLOCKS_PER_STEP and share % 128 == 0:
        packed = jnp.concatenate(
            [key_states.reshape(tokens, kv_heads * head_size), value_rows.reshape(tokens, kv_heads * head_size)], axis=1
        )
        return layer(query_states, packed, positions, out_weight, kv_heads)
    query_parts = query_states.reshape(2, half, kv_heads, group, head_size).transpose(2, 0, 3, 1, 4)
    query_parts = query_parts.reshape(kv_heads, 2, group * half, head_size)
    weight_share = lax.dynamic_slice_in_dim(out_weight, me_part * share, share, 1)
    weight = lax.all_gather(weight_share, "ctx", axis=1, tiled=True)
    packed = jnp.concatenate(
        [key_states.reshape(tokens, kv_heads * head_size), value_rows.reshape(tokens, kv_heads * head_size)], axis=1
    )
    first = positions[0] // half
    tail = jnp.broadcast_to(first.astype(packed.dtype), (TAIL, packed.shape[1]))
    gathered = spread(jnp.concatenate([packed, tail], axis=0))
    firsts = gathered[:, tokens, 0].astype(jnp.int32)
    gathered = gathered.reshape(devices * (tokens + TAIL), packed.shape[1])
    wanted = jnp.arange(blocks, dtype=jnp.int32)[:, None]
    stored = jnp.stack([firsts, blocks - 1 - firsts], axis=1).reshape(1, blocks)
    kept = jnp.arange(blocks, dtype=jnp.int32)[None, :]
    starts = kept // 2 * (tokens + TAIL) + kept % 2 * half
    place = jnp.sum(jnp.where(stored == wanted, starts, 0), axis=1)
    place = place.astype(jnp.int32)
    own = jnp.stack([first, blocks - 1 - first]).astype(jnp.int32)
    pieces = min(2, kv_heads)
    span = kv_heads // pieces
    attended = [
        attend(query_parts[i * span : (i + 1) * span], gathered, place, own, i * span, kv_heads, half) for i in range(pieces)
    ]

    def project(rows):
        product = lax.dot_general(
            jnp.concatenate(rows, axis=0), weight, (((0,), (0,)), ((), ())), preferred_element_type=jnp.float32
        )
        return product.astype(jnp.bfloat16)

    guests = [[hand_on(piece, by) for piece in attended] for by in range(1, parts)]
    mine = project(attended)
    results = [mine] + [hand_on(project(rows), parts - 1 - i) for i, rows in enumerate(guests)]
    if share % 128 == 0:
        combined = weave(results, me_part, devices)
    else:
        shares = jnp.stack([r.reshape(tokens, devices, share) for r in results])
        order = (jnp.arange(parts) - me_part) % parts
        combined = jnp.moveaxis(jnp.take(shares, order, axis=0), 0, 2).reshape(tokens, devices * parts * share)
    return lax.psum_scatter(combined, "tp", scatter_dimension=1, tiled=True)


def solution(mesh):
    in_specs = (
        P(("groups", "ctx"), "tp", None),
        P(("groups", "ctx"), "tp", None),
        P(("groups", "ctx"), "tp", None),
        P(("groups", "ctx")),
        P("tp", "ctx"),
    )
    out_specs = P(("groups", "ctx"), "tp")
    return jax.shard_map(local, mesh=mesh, in_specs=in_specs, out_specs=out_specs, check_vma=False)
```

```python
import functools
import math

import jax
import jax.numpy as jnp
from jax import lax
from jax.experimental import pallas as pl
from jax.experimental.pallas import tpu as pltpu
from jax.sharding import PartitionSpec as P

LOW_START = -1e30
BLOCKS_PER_STEP = 4
CHUNK = 1024
TAIL = 16
VMEM = 50 * 1024 * 1024


def attend_kernel(half, group, place_ref, own_ref, q_ref, k_ref, v_ref, out_ref, acc_ref, max_ref, sum_ref):
    rows = group * half
    head_size = q_ref.shape[-1]
    span = BLOCKS_PER_STEP * half
    chunk = min(CHUNK, rows)
    to_exp2 = head_size ** (-0.5) * math.log2(math.e)

    def step(which, number, masked, query_block):
        keys, values = [], []
        for i in range(BLOCKS_PER_STEP):
            place = place_ref[number * BLOCKS_PER_STEP + i]
            keys.append(k_ref[pl.ds(pl.multiple_of(place, TAIL), half), :])
            values.append(v_ref[pl.ds(pl.multiple_of(place, TAIL), half), :])
        key_part = jnp.concatenate(keys, axis=0)
        value_part = jnp.concatenate(values, axis=0)
        if masked:
            key_place = number * span + lax.broadcasted_iota(jnp.int32, (span, chunk), 0)
            query_place = query_block * half + lax.broadcasted_iota(jnp.int32, (span, chunk), 1) % half
            visible = key_place <= query_place
        for c in range(rows // chunk):
            cols = pl.ds(c * chunk, chunk)
            scores = lax.dot_general(
                key_part,
                q_ref[0, which, cols, :],
                (((1,), (1,)), ((), ())),
                preferred_element_type=jnp.float32,
            )
            if masked:
                scores = jnp.where(visible, scores, LOW_START)
            old_max = max_ref[:, cols]
            new_max = jnp.maximum(old_max, jnp.max(scores, axis=0, keepdims=True))
            factor = jnp.exp2((old_max - new_max) * to_exp2)
            exp_scores = jnp.exp2((scores - new_max) * to_exp2)
            max_ref[:, cols] = new_max
            sum_ref[:, cols] = sum_ref[:, cols] * factor + jnp.sum(exp_scores, axis=0, keepdims=True)
            weighted = lax.dot_general(
                value_part,
                exp_scores.astype(jnp.bfloat16),
                (((0,), (0,)), ((), ())),
                preferred_element_type=jnp.float32,
            )
            acc_ref[:, cols] = acc_ref[:, cols] * factor + weighted

    for which in range(2):
        query_block = own_ref[which]
        steps = query_block // BLOCKS_PER_STEP
        max_ref[...] = jnp.full_like(max_ref, LOW_START)
        sum_ref[...] = jnp.zeros_like(sum_ref)
        acc_ref[...] = jnp.zeros_like(acc_ref)

        @pl.loop(0, steps)
        def _(number):
            step(which, number, False, query_block)

        step(which, steps, True, query_block)
        for g in range(group):
            cols = pl.ds(g * half, half)
            attended = acc_ref[:, cols] / sum_ref[:, cols]
            out_ref[pl.ds(g * head_size, head_size), pl.ds(which * half, half)] = attended.astype(jnp.bfloat16)


def attend(query_parts, gathered, place, own, first_head, all_heads, half):
    kv_heads, _, rows, head_size = query_parts.shape
    keys_total = gathered.shape[0]
    blocks = place.shape[0]
    group = rows // half
    flops = 4 * kv_heads * rows * head_size * half * (blocks + 1)
    return pl.pallas_call(
        functools.partial(attend_kernel, half, group),
        out_shape=jax.ShapeDtypeStruct((kv_heads * group * head_size, 2 * half), jnp.bfloat16),
        grid_spec=pltpu.PrefetchScalarGridSpec(
            num_scalar_prefetch=2,
            grid=(kv_heads,),
            in_specs=[
                pl.BlockSpec((1, 2, rows, head_size), lambda h, *_: (h, 0, 0, 0)),
                pl.BlockSpec((keys_total, head_size), lambda h, *_: (0, h + first_head)),
                pl.BlockSpec((keys_total, head_size), lambda h, *_: (0, h + first_head + all_heads)),
            ],
            out_specs=pl.BlockSpec((group * head_size, 2 * half), lambda h, *_: (h, 0)),
            scratch_shapes=[
                pltpu.VMEM((head_size, rows), jnp.float32),
                pltpu.VMEM((1, rows), jnp.float32),
                pltpu.VMEM((1, rows), jnp.float32),
            ],
        ),
        compiler_params=pltpu.CompilerParams(
            dimension_semantics=("arbitrary",), vmem_limit_bytes=20 * 1024 * 1024
        ),
        cost_estimate=pl.CostEstimate(
            flops=flops, bytes_accessed=2 * gathered.size, transcendentals=flops // (4 * head_size)
        ),
        name="attend",
    )(place, own, query_parts, gathered, gathered)


def spread_kernel(devices, own_ref, out_ref, far_send, far_recv, side_send, side_recv, pair_send, pair_recv, own_sem):
    me = lax.axis_index("ctx")
    outers = devices // 4
    outer, middle, inner = me // 4, (me // 2) % 2, me % 2

    def at(o, m, i):
        return (o * 2 + m) * 2 + i

    side = at(outer, 1 - middle, inner)
    pair = at(outer, middle, 1 - inner)
    far = [at((outer + k) % outers, middle, inner) for k in range(1, outers)]
    barrier = pltpu.get_barrier_semaphore()
    for other in far + [side, pair]:
        pl.semaphore_signal(barrier, inc=1, device_id={"ctx": other}, device_id_type=pl.DeviceIdType.MESH)
    pl.semaphore_wait(barrier, outers + 1)

    def send(source, slot, sends, recvs, number, target):
        return pltpu.make_async_remote_copy(
            src_ref=source,
            dst_ref=out_ref.at[slot],
            send_sem=sends.at[number],
            recv_sem=recvs.at[number],
            device_id={"ctx": target},
            device_id_type=pl.DeviceIdType.MESH,
        )

    own = pltpu.make_async_copy(own_ref, out_ref.at[me], own_sem)
    far_copies = [send(own_ref, me, far_send, far_recv, k, far[k]) for k in range(outers - 1)]
    for copy in far_copies:
        copy.start()
    side_copies = [send(own_ref, me, side_send, side_recv, 0, side)]
    pair_copies = [send(own_ref, me, pair_send, pair_recv, 0, pair)]
    side_copies[0].start()
    pair_copies[0].start()
    own.start()
    for k in range(outers - 1):
        far_copies[k].wait_recv()
        slot = at((outer + outers - 1 - k) % outers, middle, inner)
        side_copies.append(send(out_ref.at[slot], slot, side_send, side_recv, k + 1, side))
        pair_copies.append(send(out_ref.at[slot], slot, pair_send, pair_recv, k + 1, pair))
        side_copies[-1].start()
        pair_copies[-1].start()
    for k in range(outers):
        side_copies[k].wait_recv()
        slot = at((outer + outers - k) % outers, 1 - middle, inner)
        pair_copies.append(send(out_ref.at[slot], slot, pair_send, pair_recv, outers + k, pair))
        pair_copies[-1].start()
    for copy in pair_copies:
        copy.wait_recv()
    for copy in far_copies + side_copies + pair_copies:
        copy.wait_send()
    own.wait()


def spread(packed):
    devices = lax.axis_size("ctx")
    outers = devices // 4
    rows, columns = packed.shape
    gathered = pl.pallas_call(
        functools.partial(spread_kernel, devices),
        out_shape=jax.ShapeDtypeStruct((devices, rows, columns), packed.dtype),
        in_specs=[pl.BlockSpec(memory_space=pltpu.VMEM)],
        out_specs=pl.BlockSpec(memory_space=pltpu.VMEM),
        scratch_shapes=[
            pltpu.SemaphoreType.DMA((outers - 1,)),
            pltpu.SemaphoreType.DMA((outers - 1,)),
            pltpu.SemaphoreType.DMA((outers,)),
            pltpu.SemaphoreType.DMA((outers,)),
            pltpu.SemaphoreType.DMA((2 * outers,)),
            pltpu.SemaphoreType.DMA((2 * outers,)),
            pltpu.SemaphoreType.DMA,
        ],
        compiler_params=pltpu.CompilerParams(
            collective_id=0, has_side_effects=True, vmem_limit_bytes=24 * 1024 * 1024
        ),
        cost_estimate=pl.CostEstimate(flops=0, bytes_accessed=20 * packed.size * devices, transcendentals=0),
        name="spread",
    )(packed)
    return gathered


def hand_on(value, by):
    parts = lax.axis_size("groups")
    return lax.ppermute(value, "groups", [(i, (i + by) % parts) for i in range(parts)])


def weave_kernel(share, me_ref, *refs):
    *shares, out_ref = refs
    parts = len(shares)
    for p in range(parts):
        by = lax.rem(p - me_ref[0] + parts, parts)
        chosen = shares[0][...]
        for k in range(1, parts):
            chosen = jnp.where(by == k, shares[k][...], chosen)
        for i in range(chosen.shape[1] // share):
            out_ref[:, (i * parts + p) * share : (i * parts + p + 1) * share] = chosen[:, i * share : (i + 1) * share]


def weave(results, me_part, devices):
    parts = len(results)
    tokens, columns = results[0].shape
    share = columns // devices
    return pl.pallas_call(
        functools.partial(weave_kernel, share),
        out_shape=jax.ShapeDtypeStruct((tokens, parts * columns), results[0].dtype),
        grid_spec=pltpu.PrefetchScalarGridSpec(
            num_scalar_prefetch=1,
            grid=(devices // 4,),
            in_specs=[pl.BlockSpec((tokens, 4 * share), lambda i, *_: (0, i))] * parts,
            out_specs=pl.BlockSpec((tokens, 4 * parts * share), lambda i, *_: (0, i)),
        ),
        name="weave",
    )(me_part.astype(jnp.int32).reshape(1), *results)


def layer_kernel(sizes, order_ref, table_ref, kv_ref, q_raw, w_ref, out_ref, *scratch):
    devices, half, kv_heads, group, head_size, share = sizes
    (kv_low, kv_high, firsts, place_vec, place_ref, w_all, acc_ref, max_ref, sum_ref, rows_ref, back_ref, part_ref, q_in, q_ref, turn_ref, *sems) = scratch
    (far_send, far_recv, side_recv, pair_send, pair_recv, wfar_send, wfar_recv, wside_send, wside_recv) = sems[:9]
    (wpair_send, wpair_recv, rows_send, rows_recv, back_send, back_recv, own_sem, place_sem, q_sem) = sems[9:]
    outers = devices // 4
    blocks = 2 * devices
    tokens = 2 * half
    width = group * half
    depth = kv_heads * group * head_size
    pieces = kv_heads
    piece = depth // pieces
    span = BLOCKS_PER_STEP * half
    groups = devices // BLOCKS_PER_STEP
    to_exp2 = head_size ** (-0.5) * math.log2(math.e)

    part = lax.axis_index("groups")
    me = lax.axis_index("ctx")
    outer, middle, inner = me // 4, (me // 2) % 2, me % 2

    def flip(number, by):
        result, unit = 0, 1
        while unit < outers:
            result = result + (number // unit + by // unit) % 2 * unit
            unit *= 2
        return result

    def slot_of(hop, cross, swap):
        return (flip(outer, hop) * 2 + (middle + cross) % 2) * 2 + (inner + swap) % 2

    far = [slot_of(k, 0, 0) for k in range(outers)]
    side = slot_of(0, 1, 0)
    pair = slot_of(0, 0, 1)
    inside = jnp.logical_and(outer > 0, outer < outers - 1)
    last = pieces - 1
    guest = lax.rem(part + 1, 2)

    barrier = pltpu.get_barrier_semaphore()
    for other in far[1:] + [side, pair]:
        pl.semaphore_signal(barrier, inc=1, device_id={"ctx": other}, device_id_type=pl.DeviceIdType.MESH)
    pl.semaphore_signal(barrier, inc=1, device_id={"groups": guest}, device_id_type=pl.DeviceIdType.MESH)
    pl.semaphore_wait(barrier, outers + 2)

    def remote(source, target, send, recv, axis, index):
        return pltpu.make_async_remote_copy(
            src_ref=source,
            dst_ref=target,
            send_sem=send,
            recv_sem=recv,
            device_id={axis: index},
            device_id_type=pl.DeviceIdType.MESH,
        )

    def own_item(item):
        return table_ref if item == 0 else kv_ref.at[pl.ds((item - 1) * half, half), :]

    def item_at(item, slot):
        if item == 0:
            return firsts.at[slot]
        return (kv_low if item == 1 else kv_high).at[slot]

    def source_of(item, hop, cross):
        return own_item(item) if hop == 0 and cross == 0 else item_at(item, slot_of(hop, cross, 0))

    def far_copy(item, hop):
        return remote(own_item(item), item_at(item, me), far_send.at[item, hop // 3], far_recv.at[item, hop], "ctx", far[hop])

    def pass_copy(item):
        ref = item_at(item, far[2])
        return remote(ref, ref, far_send.at[item, 1], far_recv.at[item, 3], "ctx", far[1])

    def side_copy(item, hop):
        return remote(
            source_of(item, hop, 0), item_at(item, far[hop]), pair_send.at[item], side_recv.at[item, hop], "ctx", side
        )

    def pair_copy(item, hop, cross):
        n = hop * 2 + cross
        return remote(
            source_of(item, hop, cross),
            item_at(item, slot_of(hop, cross, 0)),
            pair_send.at[item],
            pair_recv.at[n if item == 1 else 2 * outers + item // 2],
            "ctx",
            pair,
        )

    def w_at(slot, n):
        return w_all.at[slot, pl.ds(n * piece, piece), :]

    def far_part(hop, e):
        return w_at(slot_of(hop, 0, 0), e) if e < pieces else w_at(slot_of(hop, 1, 0), last)

    def wfar_copy(hop, e):
        ref = far_part(0, e)
        return remote(ref, ref, wfar_send.at[hop], wfar_recv.at[hop, e], "ctx", far[hop])

    def wpass_copy(e):
        ref = far_part(2, e)
        return remote(ref, ref, wfar_send.at[0], wfar_recv.at[3, e], "ctx", far[1])

    def wside_copy(hop, n):
        ref = w_at(far[hop], n)
        return remote(ref, ref, wside_send.at[min(hop, 1)], wside_recv.at[hop, n], "ctx", side)

    def wpair_copy(hop, cross, n):
        ref = w_at(slot_of(hop, cross, 0), n)
        return remote(ref, ref, wpair_send.at[hop], wpair_recv.at[hop * 2 + cross, n], "ctx", pair)

    def rows_copy(which, h):
        cols = pl.ds(pl.multiple_of(h * piece, piece), piece)
        return remote(
            rows_ref.at[pl.ds(which * half, half), cols],
            rows_ref.at[pl.ds(tokens + which * half, half), cols],
            rows_send,
            rows_recv,
            "groups",
            guest,
        )

    def back_copy(n, slot):
        cols = pl.ds(pl.multiple_of((slot * 2 + part) * share, share), share)
        return remote(back_ref.at[n], out_ref.at[:, cols], back_send, back_recv, "groups", guest)

    def all_sent(ref, sem):
        remote(ref, ref, sem, sem, "ctx", pair).wait_send()

    def all_landed(ref, sem):
        remote(ref, ref, sem, sem, "ctx", pair).wait_recv()

    def far_start(copy, hop):
        if hop == 3:

            @pl.when(inside)
            def _():
                copy.start()

        else:
            copy.start()

    def pass_on(copy):
        @pl.when(inside)
        def _():
            copy.start()

    def far_arrived(item, hop):
        far_copy(item, hop).wait_recv()
        if hop == 2:
            pass_on(pass_copy(item))
        side_copy(item, hop).start()
        pair_copy(item, hop, 0).start()

    def side_arrived(item, hop):
        side_copy(item, hop).wait_recv()
        pair_copy(item, hop, 1).start()

    def wfar_arrived(hop, e):
        wfar_copy(hop, e).wait_recv()
        if hop == 2:
            pass_on(wpass_copy(e))
        if e < last:
            wside_copy(hop, e).start()
        wpair_copy(hop, 1 if e == pieces else 0, min(e, last)).start()

    def wside_arrived(hop, n):
        wside_copy(hop, n).wait_recv()
        wpair_copy(hop, 1, n).start()

    own_weight = pltpu.make_async_copy(
        w_ref.at[:, pl.ds(pl.multiple_of(part * share, share), share)], w_all.at[me], own_sem
    )
    own_weight.start()
    queries = pltpu.make_async_copy(q_raw, q_in, q_sem)
    queries.start()
    def own_start(item):
        for hop in range(1, outers):
            far_start(far_copy(item, hop), hop)

    for item in range(2):
        side_copy(item, 0).start()
        own_start(item)
        pair_copy(item, 0, 0).start()
    pair_copy(2, 0, 0).start()
    kv_low[me] = kv_ref[:half, :]
    kv_high[me] = kv_ref[half:, :]
    firsts[me] = table_ref[...]

    def clear(at):
        max_ref[at] = jnp.full(max_ref.shape[1:], LOW_START, jnp.float32)
        sum_ref[at] = jnp.zeros(sum_ref.shape[1:], jnp.float32)
        acc_ref[at] = jnp.zeros(acc_ref.shape[1:], jnp.float32)

    for h in range(kv_heads):
        clear(h)
    queries.wait()
    for h in range(kv_heads):
        for which in range(2):
            mine = q_in[which * half : (which + 1) * half, h * group : (h + 1) * group, :]
            q_ref[h, which] = mine.reshape(width, head_size)
    own_weight.wait()

    def step(h, which, source, places, at, visible):
        keys = pl.ds(pl.multiple_of(h * head_size, head_size), head_size)
        values = pl.ds(pl.multiple_of((kv_heads + h) * head_size, head_size), head_size)
        key_part = jnp.concatenate([source[p, :, keys] for p in places], axis=0)
        value_part = jnp.concatenate([source[p, :, values] for p in places], axis=0)
        scores = lax.dot_general(
            key_part, q_ref[h, which], (((1,), (1,)), ((), ())), preferred_element_type=jnp.float32
        )
        old_max = max_ref[at]
        if visible is not None:
            scores = jnp.where(visible, scores, LOW_START)
        new_max = jnp.maximum(old_max, jnp.max(scores, axis=0, keepdims=True))
        factor = jnp.exp2((old_max - new_max) * to_exp2)
        exp_scores = jnp.exp2((scores - new_max) * to_exp2)
        max_ref[at] = new_max
        sum_ref[at] = sum_ref[at] * factor + jnp.sum(exp_scores, axis=0, keepdims=True)
        weighted = lax.dot_general(
            value_part,
            exp_scores.astype(jnp.bfloat16),
            (((0,), (0,)), ((), ())),
            preferred_element_type=jnp.float32,
        )
        acc_ref[at] = acc_ref[at] * factor + weighted

    def run_hooks(number, hooks):
        for at, actions in hooks.items():

            @pl.when(number == at)
            def _():
                for action in actions:
                    action()

    def low_blocks(parts, hooks):
        places = [slot_of(hop, cross, swap) for hop, cross in parts for swap in range(2)]
        for hop, cross in parts:
            pair_copy(1, hop, cross).wait_recv()

        @pl.loop(0, kv_heads)
        def _(h):
            run_hooks(h, hooks)
            step(h, 1, kv_low, places, h, None)

    def low_side(hop):
        for item in range(2):
            side_arrived(item, hop)

    def low_far(hop):
        for item in range(2):
            far_arrived(item, hop)

    def weight_round(e):
        for hop in (2, 1, 3):
            far_start(wfar_copy(hop, e), hop)

    def weight_own(n):
        wside_copy(0, n).start()
        wpair_copy(0, 0, n).start()

    def do(action, *args):
        return functools.partial(action, *args)

    low_side(0)
    side_copy(2, 0).start()
    low_blocks([(0, 0), (0, 1)], {2: [do(low_far, 1)]})
    low_far(2)
    own_start(2)
    low_blocks([(1, 0), (2, 0)], {})
    low_side(1)
    low_far(3)
    low_blocks([(1, 1), (3, 0)], {1: [do(low_side, 2)], 3: [do(far_arrived, 2, 1)]})
    far_arrived(2, 2)
    weight_round(0)
    low_side(3)

    def find_places():
        all_landed(firsts.at[pl.ds(0, 2 * outers)], pair_recv.at[2 * outers])
        lanes = lax.broadcasted_iota(jnp.int32, (1, half), 1)
        numbers = jnp.zeros((1, half), jnp.int32)
        for d in range(devices):
            for i in range(2):
                numbers = numbers + jnp.where(firsts[d, i : i + 1, :] // half == lanes, d, 0)
        place_vec[...] = jnp.broadcast_to(jnp.minimum(numbers, devices - 1), place_vec.shape)

    low_blocks([(2, 1), (3, 1)], {0: [do(side_arrived, 2, 0)], 1: [do(weight_own, last), find_places], 2: [do(weight_round, 1)]})
    to_scalars = pltpu.make_async_copy(place_vec, place_ref, place_sem)
    to_scalars.start()
    to_scalars.wait()

    first = order_ref[0] // half
    key_rows = lax.broadcasted_iota(jnp.int32, (span, width), 0)
    query_cols = lax.broadcasted_iota(jnp.int32, (span, width), 1) // group

    def finish(which, hooks):
        block = blocks - 1 - first if which else first

        @pl.loop(0, kv_heads)
        def _(h):
            at = h if which else kv_heads
            if not which:
                clear(at)

            @pl.loop(0, groups)
            def _(t):
                run_hooks(h * groups + t, hooks)

                @pl.when(jnp.logical_and(t == 1, h > 0))
                def _():
                    rows_copy(which, h - 1).start()

                number = groups + t if which else t
                places = [place_ref[0, number * BLOCKS_PER_STEP + i] for i in range(BLOCKS_PER_STEP)]
                visible = number * span + key_rows <= block * half + query_cols
                step(h, which, kv_high if which else kv_low, places, at, visible)

            for g in range(group):
                cols = pl.ds(g * half, half)
                attended = acc_ref[at, :, cols] / sum_ref[at, :, cols]
                turn_ref[cols, :] = attended.T
            for g in range(group):
                target = pl.ds(pl.multiple_of(h * piece + g * head_size, head_size), head_size)
                mine = turn_ref[pl.ds(g, half, stride=group), :]
                rows_ref[pl.ds(which * half, half), target] = mine.astype(jnp.bfloat16)

    def far_last(where):
        @pl.when(where)
        def _():
            wfar_arrived(2, 2)

    finish(
        0,
        {
            0: [do(weight_own, 0)],
            1: [do(side_arrived, 2, 1)],
            3: [do(far_arrived, 2, 3)],
            5: [do(side_arrived, 2, 2), do(weight_own, 1)],
            8: [do(wfar_arrived, 1, 0), do(weight_own, 2)],
            9: [do(weight_round, 2)],
            10: [do(wfar_arrived, 2, 0)],
            13: [do(wfar_arrived, 1, 1)],
            15: [do(side_arrived, 2, 3)],
        },
    )
    all_landed(kv_high.at[pl.ds(0, 2 * outers)], pair_recv.at[2 * outers + 1])
    rows_copy(0, kv_heads - 1).start()
    finish(
        1,
        {
            0: [do(wside_arrived, 0, last)],
            1: [do(wfar_arrived, 2, 1)],
            2: [do(wfar_arrived, 3, 0)],
            3: [do(weight_round, last)],
            5: [do(wside_arrived, 0, 0)],
            8: [do(wfar_arrived, 1, 2)],
            9: [do(wside_arrived, 0, 1)],
            10: [do(weight_round, pieces)],
            11: [do(far_last, inside)],
            12: [do(wfar_arrived, 3, 1)],
            13: [do(wside_arrived, 0, 2)],
            14: [do(wside_arrived, 1, 0)],
        },
    )
    wside_arrived(2, 0)
    rows_copy(1, kv_heads - 1).start()
    far_last(jnp.logical_not(inside))

    def project(hop, cross, low, high, begin=False, end=False):
        n = hop * 2 + cross
        base = slot_of(hop, cross, 0) - inner
        for m in range(low, high):
            wpair_copy(hop, cross, m).wait_recv()
        deep = pl.ds(low * piece, (high - low) * piece)
        weight = jnp.concatenate([w_all[base, deep, :], w_all[base + 1, deep, :]], axis=1)
        product = lax.dot_general(
            rows_ref[:, deep], weight, (((1,), (0,)), ((), ())), preferred_element_type=jnp.float32
        )
        if not begin:
            product = product + part_ref[n]
        if not end:
            part_ref[n] = product
            return
        product = product.astype(jnp.bfloat16)
        for i in range(2):
            back_ref[n * 2 + i] = product[tokens:, i * share : (i + 1) * share]
        for i in range(2):
            cols = pl.ds(pl.multiple_of(((base + i) * 2 + part) * share, share), share)
            out_ref[:, cols] = product[:tokens, i * share : (i + 1) * share]
        for i in range(2):
            back_copy(n * 2 + i, base + i).start()

    all_landed(rows_ref.at[pl.ds(tokens, tokens), :], rows_recv)
    project(0, 0, 0, pieces, True, True)
    wside_arrived(3, 0)
    wside_arrived(1, 1)
    wfar_arrived(3, 2)
    project(0, 1, 0, pieces, True, True)
    wfar_arrived(1, last)
    wfar_arrived(2, last)
    project(1, 0, 0, last, True)
    wside_arrived(2, 1)
    wfar_arrived(1, pieces)
    project(2, 0, 0, last, True)
    all_sent(rows_ref.at[pl.ds(0, tokens), :], rows_send)
    for item, ref in enumerate((firsts, kv_low, kv_high)):
        all_sent(ref.at[pl.ds(0, 2)], far_send.at[item, 0])
        all_sent(ref.at[pl.ds(0, 3 * outers)], pair_send.at[item])
    wfar_arrived(2, pieces)
    project(1, 0, last, pieces, False, True)
    project(2, 0, last, pieces, False, True)
    wside_arrived(1, 2)
    project(1, 1, 0, pieces, True, True)
    project(3, 0, 0, last, True)
    wside_arrived(3, 1)
    wfar_arrived(3, last)
    project(2, 1, 0, 2, True)
    project(3, 0, last, pieces, False, True)
    wside_arrived(2, 2)
    wfar_arrived(3, pieces)
    project(3, 1, 0, 1, True)
    wside_arrived(3, 2)
    project(2, 1, 2, pieces, False, True)
    project(3, 1, 1, pieces, False, True)

    @pl.when(inside)
    def _():
        for item, ref in enumerate((firsts, kv_low, kv_high)):
            all_sent(ref.at[pl.ds(0, 2)], far_send.at[item, 1])
        for i in (0, 3):
            all_sent(w_all.at[pl.ds(0, pieces + 1), pl.ds(0, piece), :], wfar_send.at[i])

    for hop in range(1, 3):
        all_sent(w_all.at[pl.ds(0, pieces + 1), pl.ds(0, piece), :], wfar_send.at[hop])
    all_sent(w_all.at[0], wside_send.at[0])
    all_sent(w_all.at[pl.ds(0, outers - 1), pl.ds(0, last * piece), :], wside_send.at[1])
    for hop in range(outers):
        all_sent(w_all.at[pl.ds(0, 2)], wpair_send.at[hop])
    all_sent(back_ref, back_send)
    all_landed(back_ref, back_recv)


def layer(query_states, packed, positions, out_weight, kv_heads):
    devices = lax.axis_size("ctx")
    outers = devices // 4
    tokens, query_heads, head_size = query_states.shape
    half = tokens // 2
    group = query_heads // kv_heads
    width = group * half
    depth, columns = out_weight.shape
    share = columns // 2
    slots = kv_heads + 1
    pieces = kv_heads
    dma = pltpu.SemaphoreType.DMA
    flops = 4 * query_states.size * half * (2 * devices + 1) // 2 + 4 * tokens * depth * columns * devices // 2
    return pl.pallas_call(
        functools.partial(layer_kernel, (devices, half, kv_heads, group, head_size, share)),
        out_shape=jax.ShapeDtypeStruct((tokens, columns * devices), jnp.bfloat16),
        in_specs=[
            pl.BlockSpec(memory_space=pltpu.SMEM),
            pl.BlockSpec(memory_space=pltpu.VMEM),
            pl.BlockSpec(memory_space=pltpu.VMEM),
            pl.BlockSpec(memory_space=pl.ANY),
            pl.BlockSpec(memory_space=pl.ANY),
        ],
        out_specs=pl.BlockSpec(memory_space=pltpu.VMEM),
        scratch_shapes=[
            pltpu.VMEM((devices, half, packed.shape[1]), packed.dtype),
            pltpu.VMEM((devices, half, packed.shape[1]), packed.dtype),
            pltpu.VMEM((devices, 2, half), jnp.int32),
            pltpu.VMEM((8, half), jnp.int32),
            pltpu.SMEM((8, half), jnp.int32),
            pltpu.VMEM((devices, depth, share), out_weight.dtype),
            pltpu.VMEM((slots, head_size, width), jnp.float32),
            pltpu.VMEM((slots, 1, width), jnp.float32),
            pltpu.VMEM((slots, 1, width), jnp.float32),
            pltpu.VMEM((2 * tokens, depth), jnp.bfloat16),
            pltpu.VMEM((devices, tokens, share), jnp.bfloat16),
            pltpu.VMEM((devices // 2, 2 * tokens, 2 * share), jnp.float32),
            pltpu.VMEM(query_states.shape, query_states.dtype),
            pltpu.VMEM((kv_heads, 2, width, head_size), query_states.dtype),
            pltpu.VMEM((width, head_size), jnp.float32),
            dma((3, 2)),
            dma((3, outers)),
            dma((3, outers)),
            dma((3,)),
            dma((2 * outers + 2,)),
            dma((outers,)),
            dma((outers, pieces + 1)),
            dma((2,)),
            dma((outers, pieces)),
            dma((outers,)),
            dma((2 * outers, pieces)),
            dma,
            dma,
            dma,
            dma,
            dma,
            dma,
            dma,
        ],
        compiler_params=pltpu.CompilerParams(
            collective_id=0, has_side_effects=True, vmem_limit_bytes=VMEM
        ),
        cost_estimate=pl.CostEstimate(flops=flops, bytes_accessed=2 * out_weight.size, transcendentals=0),
        name="layer",
    )(positions, positions.reshape(2, half), packed, query_states, out_weight)


def local(query_states, key_states, value_rows, positions, out_weight):
    tokens, query_heads, head_size = query_states.shape
    kv_heads = key_states.shape[1]
    group = query_heads // kv_heads
    half = tokens // 2
    devices = lax.axis_size("ctx")
    blocks = 2 * devices
    parts = lax.axis_size("groups")
    me_part = lax.axis_index("groups")
    share = out_weight.shape[1] // parts
    if parts == 2 and lax.axis_size("tp") == 1 and devices == 4 * BLOCKS_PER_STEP and share % 128 == 0:
        packed = jnp.concatenate(
            [key_states.reshape(tokens, kv_heads * head_size), value_rows.reshape(tokens, kv_heads * head_size)], axis=1
        )
        return layer(query_states, packed, positions, out_weight, kv_heads)
    query_parts = query_states.reshape(2, half, kv_heads, group, head_size).transpose(2, 0, 3, 1, 4)
    query_parts = query_parts.reshape(kv_heads, 2, group * half, head_size)
    weight_share = lax.dynamic_slice_in_dim(out_weight, me_part * share, share, 1)
    weight = lax.all_gather(weight_share, "ctx", axis=1, tiled=True)
    packed = jnp.concatenate(
        [key_states.reshape(tokens, kv_heads * head_size), value_rows.reshape(tokens, kv_heads * head_size)], axis=1
    )
    first = positions[0] // half
    tail = jnp.broadcast_to(first.astype(packed.dtype), (TAIL, packed.shape[1]))
    gathered = spread(jnp.concatenate([packed, tail], axis=0))
    firsts = gathered[:, tokens, 0].astype(jnp.int32)
    gathered = gathered.reshape(devices * (tokens + TAIL), packed.shape[1])
    wanted = jnp.arange(blocks, dtype=jnp.int32)[:, None]
    stored = jnp.stack([firsts, blocks - 1 - firsts], axis=1).reshape(1, blocks)
    kept = jnp.arange(blocks, dtype=jnp.int32)[None, :]
    starts = kept // 2 * (tokens + TAIL) + kept % 2 * half
    place = jnp.sum(jnp.where(stored == wanted, starts, 0), axis=1)
    place = place.astype(jnp.int32)
    own = jnp.stack([first, blocks - 1 - first]).astype(jnp.int32)
    pieces = min(2, kv_heads)
    span = kv_heads // pieces
    attended = [
        attend(query_parts[i * span : (i + 1) * span], gathered, place, own, i * span, kv_heads, half) for i in range(pieces)
    ]

    def project(rows):
        product = lax.dot_general(
            jnp.concatenate(rows, axis=0), weight, (((0,), (0,)), ((), ())), preferred_element_type=jnp.float32
        )
        return product.astype(jnp.bfloat16)

    guests = [[hand_on(piece, by) for piece in attended] for by in range(1, parts)]
    mine = project(attended)
    results = [mine] + [hand_on(project(rows), parts - 1 - i) for i, rows in enumerate(guests)]
    if share % 128 == 0:
        combined = weave(results, me_part, devices)
    else:
        shares = jnp.stack([r.reshape(tokens, devices, share) for r in results])
        order = (jnp.arange(parts) - me_part) % parts
        combined = jnp.moveaxis(jnp.take(shares, order, axis=0), 0, 2).reshape(tokens, devices * parts * share)
    return lax.psum_scatter(combined, "tp", scatter_dimension=1, tiled=True)


def solution(mesh):
    in_specs = (
        P(("groups", "ctx"), "tp", None),
        P(("groups", "ctx"), "tp", None),
        P(("groups", "ctx"), "tp", None),
        P(("groups", "ctx")),
        P("tp", "ctx"),
    )
    out_specs = P(("groups", "ctx"), "tp")
    return jax.shard_map(local, mesh=mesh, in_specs=in_specs, out_specs=out_specs, check_vma=False)
```
